256 devices in a mesh: dp: 32 (over x, y, core), mp: 8 (over z).
Axes of the slice: x: 4, y: 4, z: 8, core: 2. Of those that a mesh axis runs over, the one named last changes fastest.
Arguments:
- vit_features: bfloat16 [128, 256, 1024], P('dp', 'mp'), may hold values from -6 to 6
- patch_counts: int32 [128], P('dp'), may hold values from 64 to 192
- text_counts: int32 [128], P('dp'), may hold values from 1 to 63
- tile_dest: int32 [128], P('dp'), may hold values from 0 to 31, as said below
- text_embeds: bfloat16 [128, 256, 4096], P('dp', 'mp'), may hold values from -6 to 6
- w_proj: bfloat16 [1024, 4096], replicated, may hold values from -0.1875 to 0.1875
- b_proj: float32 [4096], replicated, may hold values from -3 to 3
- norm_gain: float32 [1, 4096], replicated, may hold values from 0.1 to 1.9
- w_qkv: bfloat16 [1, 4096, 8, 512], P(None, 'dp', 'mp'), may hold values from -0.375 to 0.375
- w_out: bfloat16 [1, 8, 256, 4096], P(None, 'mp', None, 'dp'), may hold values from -0.125 to 0.125
Outputs:
- hidden_out: bfloat16 [128, 256, 4096], P('dp', 'mp')
The draws below stay inside these ranges and needn't reach their ends.
Inputs may be any that keep to these rules, and one draw needn't show every extreme that they name: `tile_dest`: each language-model rank receives exactly 4 tiles; one source rank sends at most 2 tiles to one language-model rank, and every source rank sends 2 to some rank.
All inputs are finite; a program needn't handle non-finite values.
Results may differ from the reference program's by a relative error of at most 0.01.
Values may be sent and summed in bfloat16 or wider, within the bound.
No kernel may reach another device: no remote copies, remote signals or barrier semaphores. Data moves between devices by JAX's collectives and lax.ppermute only.
A program may use at most 128 MiB of HBM per device.

```python
import math
import jax
import jax.numpy as jnp
from jax import lax

D = 4096
VD = 1024
HS = 128
KVH = 8
GROUP = 2
LAYERS = 1
TILE = 256
IMG_DEV = 4
IMAGES = 128
N_DP = 32
N_MP = 8


def draw_tile_dest(key, part):
    rank_total = IMAGES // IMG_DEV
    owner_key = jax.random.fold_in(key, 101)
    shift_key = jax.random.fold_in(key, 202)
    order_key = jax.random.fold_in(key, 303)
    owners = jax.random.permutation(owner_key, rank_total).astype(jnp.int32)
    offsets = (1 + jax.random.permutation(shift_key, rank_total - 1)).astype(jnp.int32)
    shifts = jnp.concatenate([jnp.zeros((1,), jnp.int32), offsets[:IMG_DEV - 2], jnp.zeros((1,), jnp.int32)])
    scores = jax.random.randint(order_key, (rank_total, IMG_DEV), 0, 1 << 20) * IMG_DEV + jnp.arange(IMG_DEV, dtype=jnp.int32)[None, :]
    layers = jnp.argsort(scores, axis=1)
    picked = jnp.take(shifts, layers)
    sources = jnp.arange(rank_total, dtype=jnp.int32)[:, None]
    destinations = jnp.take(owners, (sources + picked) % rank_total)
    return destinations.reshape(IMAGES).astype(jnp.int32)


def draw_w_qkv(key, part):
    base_key = jax.random.fold_in(key, 404)
    width_all = (GROUP + 2) * HS
    base = jax.random.truncated_normal(base_key, -4.0, 4.0, (LAYERS, D, KVH, width_all), jnp.float32) * D ** (-0.5)
    return base.astype(jnp.bfloat16)


def set_ends(result, own_key, smallest, largest):
    spot = [jax.random.randint(jax.random.fold_in(own_key, axis), (), 0, length) for axis, length in enumerate(result.shape)]
    longest = result.shape.index(max(result.shape))
    neighbour = spot[:longest] + [(spot[longest] + 1) % result.shape[longest]] + spot[longest + 1:]
    return result.at[tuple(spot)].set(smallest).at[tuple(neighbour)].set(largest)


def levels(rng, shape, cuts, smallest, top_value):
    factor_of, own = 1.0, jax.random.fold_in(rng, 6)
    for axis_at, parts in cuts:
        draws = jnp.exp(jax.random.uniform(jax.random.fold_in(own, axis_at), (parts,), jnp.float32, smallest / len(cuts), top_value / len(cuts)))
        factor_of = factor_of * jnp.repeat(draws, shape[axis_at] // parts).reshape([-1 if axis == axis_at else 1 for axis in range(len(shape))])
    return factor_of


def noise(rng, extent, width, bound, cuts=(), kind=jnp.bfloat16):
    array = jax.random.normal(rng, extent, jnp.float32) * width
    if len(cuts) > 0:
        array = levels(rng, extent, cuts, -0.22, 0.18) * array
    return jnp.clip(array, min=-bound, max=bound).astype(kind)


def setup_inputs(seed: int = 0) -> dict:
    keys = jax.random.split(jax.random.key(seed), 11)
    return {
        "vit_features": noise(keys[0], (IMAGES, TILE, VD), 1.0, 6.0, ((0, 32), (1, 8))),
        "patch_counts": set_ends(jax.random.randint(keys[1], (IMAGES,), TILE // 4, 3 * TILE // 4 + 1), jax.random.fold_in(keys[1], 1), TILE // 4, (3 * TILE // 4 + 1) - 1).astype(jnp.int32),
        "text_counts": set_ends(jax.random.randint(keys[2], (IMAGES,), 1, TILE // 4), jax.random.fold_in(keys[2], 1), 1, (TILE // 4) - 1).astype(jnp.int32),
        "tile_dest": draw_tile_dest(jax.random.fold_in(keys[10], 71), 0),
        "text_embeds": noise(keys[4], (IMAGES, TILE, D), 1.0, 6.0, ((0, 32), (1, 8))),
        "w_proj": noise(keys[5], (VD, D), VD ** -0.5, 0.1875),
        "b_proj": noise(keys[6], (D,), 0.5, 3.0, (), jnp.float32),
        "norm_gain": jnp.clip(1.0 + 0.18 * jax.random.normal(keys[7], (LAYERS, D), jnp.float32), 0.1, 1.9),
        "w_qkv": draw_w_qkv(jax.random.fold_in(keys[10], 71), 0),
        "w_out": noise(keys[9], (LAYERS, KVH, GROUP * HS, D), (KVH * GROUP * HS) ** -0.5, 0.125, ((1, 8), (3, 32))),
    }


rope_base = 500000.0
epsilon = 1e-05

def tile_angles(tile_size, head_size):
    half_size = head_size // 2
    inverse = jnp.exp(-(2.0 * jnp.arange(half_size, dtype=jnp.float32) / head_size) * math.log(rope_base))
    positions = jnp.arange(tile_size, dtype=jnp.float32)
    return positions[:, None] * inverse[None, :]

def rotate_half(values, angles):
    half_size = values.shape[-1] // 2
    cosine = jnp.cos(angles)
    sine_part = jnp.sin(angles)
    first_half = values[..., :half_size]
    second = values[..., half_size:]
    return jnp.concatenate([first_half * cosine - second * sine_part, second * cosine + first_half * sine_part], axis=-1)

def attend_tile(operands):
    tile_queries, tile_keys, tile_values, length = operands
    score_scale = 1.0 / math.sqrt(HS)
    scores = jnp.einsum('rhge,che->hgrc', tile_queries.astype(jnp.float32), tile_keys.astype(jnp.float32)) * score_scale
    row_ids = jnp.arange(TILE, dtype=jnp.int32)[:, None]
    col_ids = jnp.arange(TILE, dtype=jnp.int32)[None, :]
    allowed = (col_ids <= row_ids) & (col_ids < length)
    scores = jnp.where(allowed, scores, -1e+30)
    row_max = lax.optimization_barrier(jnp.max(scores, axis=-1, keepdims=True))
    weights = jnp.where(allowed, jnp.exp(scores - row_max), 0.0)
    probabilities = (weights / lax.optimization_barrier(jnp.sum(weights, axis=-1, keepdims=True))).astype(jnp.bfloat16)
    return jnp.einsum('hgrc,che->rhge', probabilities.astype(jnp.float32), tile_values.astype(jnp.float32)).astype(jnp.bfloat16)

def decoder_attention(hidden, gain_row, weights_qkv, weights_out, lengths, angles):
    image_total = hidden.shape[0]
    as_float = hidden.astype(jnp.float32)
    mean_square = lax.optimization_barrier(jnp.mean(as_float * as_float, axis=-1, keepdims=True))
    normed = (as_float * lax.rsqrt(mean_square + epsilon) * gain_row).astype(jnp.bfloat16)
    joined_rows = jnp.dot(normed.reshape(image_total * TILE, D), weights_qkv.reshape(D, KVH * (GROUP + 2) * HS), preferred_element_type=jnp.float32)
    joined_rows = joined_rows.reshape(image_total, TILE, KVH, GROUP + 2, HS)
    queries = rotate_half(joined_rows[:, :, :, :GROUP, :], angles[None, :, None, None, :]).astype(jnp.bfloat16)
    key_heads = rotate_half(joined_rows[:, :, :, GROUP, :], angles[None, :, None, :]).astype(jnp.bfloat16)
    value_heads = joined_rows[:, :, :, GROUP + 1, :].astype(jnp.bfloat16)
    attended = lax.map(attend_tile, (queries, key_heads, value_heads, lengths))
    attended = attended.reshape(image_total * TILE, KVH * GROUP * HS)
    out_rows = weights_out.reshape(KVH * GROUP * HS, D)
    shard_width = KVH // N_MP * GROUP * HS
    summed = jnp.zeros((image_total * TILE, D), jnp.float32)
    for shard_idx in range(N_MP):
        partial_sum = jnp.dot(attended[:, shard_idx * shard_width:(shard_idx + 1) * shard_width], out_rows[shard_idx * shard_width:(shard_idx + 1) * shard_width], preferred_element_type=jnp.float32)
        summed = summed + lax.optimization_barrier(partial_sum.astype(jnp.bfloat16)).astype(jnp.float32)
    return (as_float + summed.reshape(image_total, TILE, D)).astype(jnp.bfloat16)

def reference(vit_features, patch_counts, text_counts, tile_dest, text_embeds, w_proj, b_proj, norm_gain, w_qkv, w_out):
    image_total = tile_dest.shape[0]
    dest_ids = jnp.arange(N_DP, dtype=jnp.int32)
    dest_hot = (tile_dest[:, None] == dest_ids[None, :]).astype(jnp.int32)
    earlier = jnp.cumsum(dest_hot, axis=0) - dest_hot
    slot_ids = lax.optimization_barrier(jnp.sum(earlier * dest_hot, axis=1)).astype(jnp.int32)
    targets = (tile_dest * IMG_DEV + slot_ids).astype(jnp.int32)
    sources = jnp.zeros((image_total,), jnp.int32).at[targets].set(jnp.arange(image_total, dtype=jnp.int32))
    placed = jnp.take(vit_features, sources, axis=0)
    projected = jnp.dot(placed.reshape(image_total * TILE, VD), w_proj, preferred_element_type=jnp.float32) + b_proj
    projected = projected.reshape(image_total, TILE, D)
    row_ids = jnp.arange(TILE, dtype=jnp.int32)[None, :, None]
    image_end = patch_counts[:, None, None]
    text_end = (patch_counts + text_counts)[:, None, None]
    hidden = jnp.where(row_ids < image_end, projected, jnp.where(row_ids < text_end, text_embeds.astype(jnp.float32), 0.0)).astype(jnp.bfloat16)
    lengths = patch_counts + text_counts
    angles = tile_angles(TILE, HS)
    for layer_idx in range(LAYERS):
        hidden = decoder_attention(hidden, norm_gain[layer_idx], w_qkv[layer_idx], w_out[layer_idx], lengths, angles)
    return hidden
```

```python
import math

import jax
import jax.numpy as jnp
from jax import lax
from jax.experimental import pallas as pl
from jax.experimental.pallas import tpu as pltpu
from jax.sharding import PartitionSpec as P

HS = 128
GROUP = 2
WINDOW = 64
EXTRA = 128

rope_base = 500000.0
epsilon = 1e-05


def shifted(value, axis, step):
    size = lax.axis_size(axis)
    return lax.ppermute(value, axis, [(i, (i + step) % size) for i in range(size)])


def ring_chunks(own, axis):
    size = lax.axis_size(axis)
    chunks = [own] + [None] * (size - 1)
    for s in range(1, size // 2 + 1):
        chunks[s] = shifted(chunks[s - 1], axis, 1)
        if s < size - s:
            chunks[size - s] = shifted(chunks[(size - s + 1) % size], axis, -1)
    return chunks


def rms_normed(hidden, gain):
    as_float = hidden.astype(jnp.float32)
    mean_square = jnp.mean(as_float * as_float, axis=-1, keepdims=True)
    return (as_float * lax.rsqrt(mean_square + epsilon) * gain).astype(jnp.bfloat16)


def angles_of(rows):
    half_size = HS // 2
    inverse = jnp.exp(
        -(2.0 * jnp.arange(half_size, dtype=jnp.float32) / HS) * math.log(rope_base)
    )
    return rows.astype(jnp.float32)[..., None] * inverse


def rotated(values, cosine, sine):
    half_size = HS // 2
    first_half = values[..., :half_size]
    second = values[..., half_size:]
    return jnp.concatenate(
        [first_half * cosine - second * sine, second * cosine + first_half * sine], axis=-1
    )


def rotated_qkv(joined, rows):
    angles = angles_of(rows)
    cosine, sine = jnp.cos(angles)[..., None, :], jnp.sin(angles)[..., None, :]
    parts = joined.reshape(*joined.shape[:-1], GROUP + 2, HS)
    turned = rotated(parts[..., : GROUP + 1, :], cosine, sine)
    return (
        jnp.concatenate([turned, parts[..., GROUP + 1 :, :]], axis=-2)
        .reshape(joined.shape)
        .astype(jnp.bfloat16)
    )


def exchange_tiles(vit_features, tile_dest):
    image_count, local_rows, width = vit_features.shape
    ranks = lax.axis_size("dp")
    rows_per = local_rows // ranks
    by_row = jnp.moveaxis(vit_features.reshape(image_count, ranks, rows_per * width), 1, 0)
    tags = jnp.broadcast_to(
        tile_dest.astype(jnp.bfloat16)[None, :, None], (ranks, image_count, EXTRA)
    )
    sent = jnp.concatenate([by_row, tags], axis=2)
    got = lax.all_to_all(sent, "dp", split_axis=0, concat_axis=0, tiled=True)
    total = ranks * image_count
    got = got.reshape(total, rows_per * width + EXTRA)
    dest = got[:, rows_per * width : rows_per * width + 1].astype(jnp.float32)
    ids = jnp.arange(total, dtype=jnp.int32)
    same = dest == dest.reshape(1, total)
    earlier = same & (ids[None, :] < ids[:, None])
    slots = jnp.sum(earlier.astype(jnp.float32), axis=1, keepdims=True)
    targets = (dest * image_count + slots).astype(jnp.int32)
    placing = (targets == ids[None, :]).astype(jnp.bfloat16)
    ordered = lax.dot_general(
        placing,
        got[:, : rows_per * width],
        (((0,), (0,)), ((), ())),
        preferred_element_type=jnp.float32,
    ).astype(jnp.bfloat16)
    arrived = lax.all_to_all(
        ordered.reshape(ranks, image_count, rows_per * width),
        "dp",
        split_axis=0,
        concat_axis=0,
        tiled=True,
    )
    return jnp.moveaxis(arrived, 0, 1).reshape(image_count, local_rows, width)


def text_windows(text_embeds, patch_counts, text_counts):
    image_count, local_rows, model_width = text_embeds.shape
    parts = lax.axis_size("mp")
    slice_width = model_width // parts
    columns = jnp.moveaxis(
        text_embeds.reshape(image_count, local_rows, parts, slice_width), 2, 0
    )
    columns = lax.all_to_all(columns, "mp", split_axis=0, concat_axis=0, tiled=True)
    tile_rows = jnp.moveaxis(columns, 0, 1).reshape(image_count, parts * local_rows, slice_width)
    places = jnp.arange(WINDOW, dtype=jnp.int32)[None, :, None]
    rows = jnp.arange(parts * local_rows, dtype=jnp.int32)[None, None, :]
    picks = (
        (rows == patch_counts[:, None, None] + places) & (places < text_counts[:, None, None])
    ).astype(jnp.bfloat16)
    window = jnp.einsum(
        "tir,trk->tik", picks, tile_rows, preferred_element_type=jnp.float32
    ).astype(jnp.bfloat16)
    window = window.reshape(image_count * WINDOW, slice_width)
    mine = lax.axis_index("mp")
    whole = jnp.zeros((parts, *window.shape), jnp.bfloat16)
    for s, chunk in enumerate(ring_chunks(window, "mp")):
        whole = lax.dynamic_update_index_in_dim(whole, chunk, lax.rem(mine + (parts - s), parts), 0)
    return jnp.moveaxis(whole, 0, 1).reshape(image_count * WINDOW, model_width)


def attend(qkv, row_ids, lengths):
    tiles, rows = qkv.shape[:2]
    parts = qkv.reshape(tiles, rows, GROUP + 2, HS)
    queries, keys, values = parts[:, :, :GROUP], parts[:, :, GROUP], parts[:, :, GROUP + 1]
    scores = jnp.einsum(
        "brge,bce->bgrc", queries, keys, preferred_element_type=jnp.float32
    ) * (1.0 / math.sqrt(HS))
    allowed = (row_ids[None, :] <= row_ids[:, None])[None, None] & (
        row_ids[None, None, None, :] < lengths[:, None, None, None]
    )
    scores = jnp.where(allowed, scores, -1e30)
    row_max = jnp.max(scores, axis=-1, keepdims=True)
    weights = jnp.where(allowed, jnp.exp(scores - row_max), 0.0)
    probabilities = (weights / jnp.sum(weights, axis=-1, keepdims=True)).astype(jnp.bfloat16)
    return jnp.einsum(
        "bgrc,bce->brge", probabilities, values, preferred_element_type=jnp.float32
    ).astype(jnp.bfloat16).reshape(tiles, rows, GROUP * HS)


def out_kernel(att_ref, weight_ref, hidden_ref, out_ref):
    for j in range(weight_ref.shape[0]):
        width = weight_ref.shape[2]
        cols = slice(j * width, (j + 1) * width)
        total = jnp.dot(att_ref[...], weight_ref[j], preferred_element_type=jnp.float32)
        out_ref[:, cols] = (hidden_ref[:, cols].astype(jnp.float32) + total).astype(jnp.bfloat16)


def project_out(attended, weight_blocks, hidden):
    rows, depth = attended.shape
    blocks, _, width = weight_blocks.shape
    step = 4
    return pl.pallas_call(
        out_kernel,
        grid=(blocks // step,),
        in_specs=[
            pl.BlockSpec((rows, depth), lambda i: (0, 0)),
            pl.BlockSpec((step, depth, width), lambda i: (i, 0, 0)),
            pl.BlockSpec((rows, step * width), lambda i: (0, i)),
        ],
        out_specs=pl.BlockSpec((rows, step * width), lambda i: (0, i)),
        out_shape=jax.ShapeDtypeStruct((rows, blocks * width), jnp.bfloat16),
        compiler_params=pltpu.CompilerParams(dimension_semantics=("arbitrary",)),
        cost_estimate=pl.CostEstimate(
            flops=2 * rows * depth * blocks * width,
            bytes_accessed=2 * depth * blocks * width,
            transcendentals=0,
        ),
    )(attended, weight_blocks, hidden)


def body(
    vit_features,
    patch_counts,
    text_counts,
    tile_dest,
    text_embeds,
    w_proj,
    b_proj,
    norm_gain,
    w_qkv,
    w_out,
):
    parts = lax.axis_size("mp")
    mine = lax.axis_index("mp")
    image_count, local_rows, _ = vit_features.shape
    model_width = text_embeds.shape[-1]
    gain = norm_gain[0]
    lengths = patch_counts + text_counts

    all_qkv = lax.all_gather(w_qkv[0, :, 0], "dp", axis=0, tiled=True)
    head_rows = jnp.concatenate(
        [w_out[0, 0]] + [shifted(w_out[0, 0], "mp", -s) for s in range(1, parts)], axis=0
    )
    all_out = lax.all_gather(head_rows[None], "dp", axis=0, tiled=True)

    text_rows = text_windows(text_embeds, patch_counts, text_counts)
    text_joined = jnp.dot(
        rms_normed(text_rows, gain), all_qkv, preferred_element_type=jnp.float32
    )
    text_places = (patch_counts[:, None] + jnp.arange(WINDOW, dtype=jnp.int32)[None, :])
    text_qkv = rotated_qkv(
        text_joined.reshape(image_count, WINDOW, -1), text_places
    )

    arrived = exchange_tiles(vit_features, tile_dest)
    chunks = ring_chunks(arrived, "mp")

    own_rows = mine * local_rows + jnp.arange(local_rows, dtype=jnp.int32)
    chunk_rows = jnp.stack(
        [lax.rem(mine + (parts - s), parts) * local_rows + jnp.arange(local_rows, dtype=jnp.int32) for s in range(parts)]
    )

    def project(rows):
        flat = rows.reshape(-1, rows.shape[-1])
        return (
            jnp.dot(flat, w_proj, preferred_element_type=jnp.float32) + b_proj
        ).astype(jnp.bfloat16)

    groups = [[0]] + [[s, parts - s] for s in range(1, parts // 2 - 1)] + [
        [parts // 2 - 1, parts // 2 + 1, parts // 2]
    ]
    joined_of = [None] * parts
    own_projected = None
    for group in groups:
        stacked = jnp.stack([chunks[s] for s in group])
        projected = project(stacked)
        if group == [0]:
            own_projected = projected.reshape(image_count, local_rows, model_width)
        joined = jnp.dot(
            rms_normed(projected, gain), all_qkv, preferred_element_type=jnp.float32
        ).reshape(len(group), image_count, local_rows, -1)
        for at, s in enumerate(group):
            joined_of[s] = joined[at]
    image_joined = jnp.stack(joined_of)
    image_qkv = rotated_qkv(image_joined, jnp.broadcast_to(chunk_rows[:, None, :], image_joined.shape[:3]))
    image_qkv = jnp.moveaxis(image_qkv, 0, 1).reshape(image_count, parts * local_rows, -1)
    flat_rows = chunk_rows.reshape(-1)
    placing = (flat_rows[None, :, None] == text_places[:, None, :]).astype(jnp.bfloat16)
    placed_text = jnp.einsum(
        "tri,tik->trk", placing, text_qkv, preferred_element_type=jnp.float32
    ).astype(jnp.bfloat16)
    is_text = flat_rows[None, :, None] < lengths[:, None, None]
    qkv = jnp.where(
        flat_rows[None, :, None] < patch_counts[:, None, None],
        image_qkv,
        jnp.where(is_text, placed_text, jnp.zeros_like(placed_text)),
    )

    hidden = jnp.where(
        own_rows[None, :, None] < patch_counts[:, None, None],
        own_projected,
        jnp.where(
            own_rows[None, :, None] < lengths[:, None, None],
            text_embeds,
            jnp.zeros_like(text_embeds),
        ),
    ).reshape(image_count * local_rows, model_width)

    attended = attend(qkv, flat_rows, lengths)
    attended = attended.reshape(image_count, parts, local_rows, -1)
    returned = [
        attended[:, 0] if s == 0 else shifted(attended[:, s], "mp", -s) for s in range(parts)
    ]
    returned = jnp.concatenate(
        [r.reshape(image_count * local_rows, -1) for r in returned], axis=1
    )
    out = project_out(returned, all_out, hidden)
    return out.reshape(image_count, local_rows, model_width)


def solution(mesh):
    in_specs = (
        P("dp", "mp", None),
        P("dp"),
        P("dp"),
        P("dp"),
        P("dp", "mp", None),
        P(),
        P(),
        P(),
        P(None, "dp", "mp", None),
        P(None, "mp", None, "dp"),
    )
    out_specs = P("dp", "mp", None)
    return jax.shard_map(body, mesh=mesh, in_specs=in_specs, out_specs=out_specs, check_vma=False)
```

```python
import functools
import math

import jax
import jax.numpy as jnp
from jax import lax
from jax.experimental import pallas as pl
from jax.experimental.pallas import tpu as pltpu
from jax.sharding import PartitionSpec as P


HS = 128
GROUP = 2
WINDOW = 64
EXTRA = 128

rope_base = 500000.0
epsilon = 1e-05


def shifted(value, axis, step):
    size = lax.axis_size(axis)
    return lax.ppermute(value, axis, [(i, (i + step) % size) for i in range(size)])


def ring_chunks(own, axis):
    size = lax.axis_size(axis)
    chunks = [own] + [None] * (size - 1)
    for s in range(1, size // 2 + 1):
        chunks[s] = shifted(chunks[s - 1], axis, 1)
        if s < size - s:
            chunks[size - s] = shifted(chunks[(size - s + 1) % size], axis, -1)
    return chunks


def rotation_tables(rows):
    half_size = HS // 2
    inverse = jnp.exp(
        -(2.0 * jnp.arange(half_size, dtype=jnp.float32) / HS) * math.log(rope_base)
    )
    angles = rows.astype(jnp.float32)[..., None] * inverse
    cosine, sine = jnp.cos(angles), jnp.sin(angles)
    return (
        jnp.concatenate([cosine, cosine], axis=-1),
        jnp.concatenate([-sine, sine], axis=-1),
    )


def rotate_store(joined, cosine, sine, store):
    heads = joined.shape[1] // HS
    for p in range(heads):
        part = joined[:, p * HS : (p + 1) * HS]
        if p < heads - 1:
            part = part * cosine + pltpu.roll(part, HS // 2, 1) * sine
        store(p, part.astype(jnp.bfloat16))


def order_kernel(got_ref, out_ref, *, image_count):
    total, wide = got_ref.shape
    width = wide - EXTRA
    dest = got_ref[:, width:].astype(jnp.float32)
    row = lax.broadcasted_iota(jnp.int32, (total, total), 0)
    col = lax.broadcasted_iota(jnp.int32, (total, total), 1)
    earlier = (dest == dest.T) & (col < row)
    slots = jnp.sum(jnp.where(earlier, 1.0, 0.0), axis=1, keepdims=True)
    targets = (dest * image_count + slots).T
    placing = jnp.where(targets == row.astype(jnp.float32), 1.0, 0.0).astype(jnp.bfloat16)
    out_ref[...] = jnp.dot(
        placing, got_ref[:, :width], preferred_element_type=jnp.float32
    ).astype(jnp.bfloat16)


def exchange_tiles(vit_features, tile_dest):
    image_count, _, width = vit_features.shape
    ranks = lax.axis_size("dp")
    by_row = jnp.moveaxis(vit_features, 1, 0)
    tags = jnp.broadcast_to(
        tile_dest.astype(jnp.bfloat16)[None, :, None], (ranks, image_count, EXTRA)
    )
    sent = jnp.concatenate([by_row, tags], axis=2)
    got = lax.all_to_all(sent, "dp", split_axis=0, concat_axis=0, tiled=True)
    total = ranks * image_count
    ordered = pl.pallas_call(
        functools.partial(order_kernel, image_count=image_count),
        out_shape=jax.ShapeDtypeStruct((total, width), jnp.bfloat16),
        cost_estimate=pl.CostEstimate(
            flops=2 * total * total * width, bytes_accessed=4 * total * width, transcendentals=0
        ),
    )(got.reshape(total, width + EXTRA))
    arrived = lax.all_to_all(
        ordered.reshape(ranks, image_count, width),
        "dp",
        split_axis=0,
        concat_axis=0,
        tiled=True,
    )
    return jnp.moveaxis(arrived, 0, 1)


def pack_kernel(place_ref, text_ref, heads_ref, *out_refs):
    parts = len(out_refs)
    rows, wide = out_refs[0].shape
    folds = heads_ref.shape[0] // rows
    cols = heads_ref.shape[1]
    width = wide - folds * cols
    mine = place_ref[0]
    for s, out_ref in enumerate(out_refs):
        at = pl.multiple_of(lax.rem(mine + s, parts) * width, width)
        out_ref[:, :width] = text_ref[:, :, pl.ds(at, width)].reshape(rows, width)
        for f in range(folds):
            out_ref[:, width + f * cols : width + (f + 1) * cols] = heads_ref[
                f * rows : (f + 1) * rows, :
            ]


def pack(text_embeds, head_rows, mine, parts):
    tiles, local_rows, model_width = text_embeds.shape
    rows = tiles * local_rows
    width = model_width // parts
    wide = width + head_rows.shape[0] * head_rows.shape[1] // rows
    whole = pl.BlockSpec(memory_space=pltpu.VMEM)
    return pl.pallas_call(
        pack_kernel,
        in_specs=[pl.BlockSpec(memory_space=pltpu.SMEM), whole, whole],
        out_specs=[whole] * parts,
        out_shape=[jax.ShapeDtypeStruct((rows, wide), jnp.bfloat16)] * parts,
        cost_estimate=pl.CostEstimate(
            flops=1 << 20, bytes_accessed=4 * parts * rows * wide, transcendentals=0
        ),
    )(mine.reshape(1), text_embeds, head_rows)


def unpack_kernel(counts_ref, *refs, tiles, width):
    parts = len(refs) - 3
    got_refs = refs[:parts]
    window_ref, heads_ref, rows_ref = refs[parts:]
    mine = counts_ref[2, 0]
    each, wide = got_refs[0].shape
    local_rows = each // tiles
    cols = heads_ref.shape[1]
    folds = (wide - width) // cols
    for s, got_ref in enumerate(got_refs):
        at = lax.rem(mine + (parts - s), parts)
        for f in range(folds):
            begin = pl.multiple_of((at * folds + f) * each, each)
            heads_ref[pl.ds(begin, each), :] = got_ref[:, width + f * cols : width + (f + 1) * cols]
        for t in range(tiles):
            rows_ref[t, at] = got_ref[t * local_rows : (t + 1) * local_rows, :width]
    rows = parts * local_rows
    place = lax.broadcasted_iota(jnp.int32, (WINDOW, rows), 0)
    row = lax.broadcasted_iota(jnp.int32, (WINDOW, rows), 1)
    for t in range(tiles):
        picks = (row == counts_ref[0, t] + place) & (place < counts_ref[1, t])
        window_ref[t * WINDOW : (t + 1) * WINDOW, :] = jnp.dot(
            jnp.where(picks, 1.0, 0.0).astype(jnp.bfloat16),
            rows_ref[t].reshape(rows, width),
            preferred_element_type=jnp.float32,
        ).astype(jnp.bfloat16)


def unpack(got, counts, tiles, width, cols):
    parts = len(got)
    each, wide = got[0].shape
    local_rows = each // tiles
    whole = pl.BlockSpec(memory_space=pltpu.VMEM)
    return pl.pallas_call(
        functools.partial(unpack_kernel, tiles=tiles, width=width),
        in_specs=[pl.BlockSpec(memory_space=pltpu.SMEM)] + [whole] * parts,
        out_specs=[whole, whole],
        out_shape=[
            jax.ShapeDtypeStruct((tiles * WINDOW, width), jnp.bfloat16),
            jax.ShapeDtypeStruct((parts * each * ((wide - width) // cols), cols), jnp.bfloat16),
        ],
        scratch_shapes=[pltpu.VMEM((tiles, parts, local_rows, width), jnp.bfloat16)],
        cost_estimate=pl.CostEstimate(
            flops=2 * tiles * WINDOW * parts * local_rows * width,
            bytes_accessed=2 * parts * each * wide,
            transcendentals=0,
        ),
    )(counts, *got)


def text_kernel(place_ref, *refs):
    parts = len(refs) - 5
    chunk_refs = refs[:parts]
    cos_ref, sin_ref, gain_ref, weight_ref, out_ref = refs[parts:]
    width = chunk_refs[0].shape[1]
    mine = place_ref[0]
    squares = None
    total = None
    for s, chunk_ref in enumerate(chunk_refs):
        at = lax.rem(mine + (parts - s), parts)
        rows = chunk_ref[...].astype(jnp.float32)
        part = jnp.sum(rows * rows, axis=1, keepdims=True)
        squares = part if squares is None else squares + part
        scaled = (rows * gain_ref[pl.ds(at, 1), :]).astype(jnp.bfloat16)
        block = weight_ref[pl.ds(pl.multiple_of(at * width, width), width), :]
        term = jnp.dot(scaled, block, preferred_element_type=jnp.float32)
        total = term if total is None else total + term
    scale = lax.rsqrt(squares * (1.0 / (parts * width)) + epsilon)

    def store(p, value):
        out_ref[:, p * HS : (p + 1) * HS] = value

    rotate_store(total * scale, cos_ref[...], sin_ref[...], store)


def text_qkv_of(chunks, mine, cosine, sine, gain, all_qkv):
    rows, width = chunks[0].shape
    parts = len(chunks)
    outs = all_qkv.shape[1]
    whole = pl.BlockSpec(memory_space=pltpu.VMEM)
    return pl.pallas_call(
        text_kernel,
        in_specs=[pl.BlockSpec(memory_space=pltpu.SMEM)] + [whole] * (parts + 4),
        out_specs=whole,
        out_shape=jax.ShapeDtypeStruct((rows, outs), jnp.bfloat16),
        cost_estimate=pl.CostEstimate(
            flops=2 * rows * parts * width * outs,
            bytes_accessed=2 * parts * width * (rows + outs),
            transcendentals=0,
        ),
    )(mine.reshape(1), *chunks, cosine, sine, gain.reshape(parts, width), all_qkv)


def image_kernel(*refs, groups, with_hidden):
    chunk_refs = refs[:groups]
    cos_ref, sin_ref, proj_ref, bias_ref, gain_ref, qkv_ref = refs[groups : groups + 6]
    out_ref = refs[groups + 6]
    hidden_ref = refs[groups + 7] if with_hidden else None
    rows_ref, sum_ref, squares_ref = refs[-3:]
    tiles, local_rows, depth = chunk_refs[0].shape
    each = tiles * local_rows
    step = pl.program_id(0)

    @pl.when(step == 0)
    def _():
        for g, chunk_ref in enumerate(chunk_refs):
            rows_ref[g * each : (g + 1) * each, :] = chunk_ref[...].reshape(each, depth)
        sum_ref[...] = jnp.zeros_like(sum_ref)
        squares_ref[...] = jnp.zeros_like(squares_ref)

    projected = (
        jnp.dot(rows_ref[...], proj_ref[...], preferred_element_type=jnp.float32) + bias_ref[...]
    ).astype(jnp.bfloat16)
    if with_hidden:
        hidden_ref[...] = projected[:each]
    wide = projected.astype(jnp.float32)
    squares_ref[...] += jnp.sum(wide * wide, axis=1, keepdims=True)
    scaled = (wide * gain_ref[...]).astype(jnp.bfloat16)
    sum_ref[...] += jnp.dot(scaled, qkv_ref[...], preferred_element_type=jnp.float32)

    @pl.when(step == pl.num_programs(0) - 1)
    def _():
        model_width = proj_ref.shape[1] * pl.num_programs(0)
        scale = lax.rsqrt(squares_ref[...] * (1.0 / model_width) + epsilon)
        shape = (groups, tiles, local_rows, HS)
        cosine = jnp.broadcast_to(cos_ref[...][:, None], shape).reshape(groups * each, HS)
        sine = jnp.broadcast_to(sin_ref[...][:, None], shape).reshape(groups * each, HS)

        def store(p, value):
            out_ref[:, :, :, p * HS : (p + 1) * HS] = value.reshape(shape)

        rotate_store(sum_ref[...] * scale, cosine, sine, store)


def image_qkv_of(chunks, cosine, sine, w_proj, bias, gain, all_qkv, with_hidden):
    groups = len(chunks)
    tiles, local_rows, depth = chunks[0].shape
    model_width, outs = all_qkv.shape
    each = tiles * local_rows
    block = 512
    fixed = lambda *shape: pl.BlockSpec(shape, lambda i: (0,) * len(shape))
    out_specs = [fixed(groups, tiles, local_rows, outs)]
    out_shape = [jax.ShapeDtypeStruct((groups, tiles, local_rows, outs), jnp.bfloat16)]
    if with_hidden:
        out_specs.append(pl.BlockSpec((each, block), lambda i: (0, i)))
        out_shape.append(jax.ShapeDtypeStruct((each, model_width), jnp.bfloat16))
    return pl.pallas_call(
        functools.partial(image_kernel, groups=groups, with_hidden=with_hidden),
        grid=(model_width // block,),
        in_specs=[fixed(tiles, local_rows, depth)] * groups
        + [
            fixed(groups, local_rows, HS),
            fixed(groups, local_rows, HS),
            pl.BlockSpec((depth, block), lambda i: (0, i)),
            pl.BlockSpec((1, block), lambda i: (0, i)),
            pl.BlockSpec((1, block), lambda i: (0, i)),
            pl.BlockSpec((block, outs), lambda i: (i, 0)),
        ],
        out_specs=out_specs,
        out_shape=out_shape,
        scratch_shapes=[
            pltpu.VMEM((groups * each, depth), jnp.bfloat16),
            pltpu.VMEM((groups * each, outs), jnp.float32),
            pltpu.VMEM((groups * each, 1), jnp.float32),
        ],
        compiler_params=pltpu.CompilerParams(dimension_semantics=("arbitrary",)),
        cost_estimate=pl.CostEstimate(
            flops=2 * groups * each * model_width * (depth + outs),
            bytes_accessed=2 * model_width * (depth + outs),
            transcendentals=0,
        ),
    )(*chunks, cosine, sine, w_proj, bias, gain, all_qkv)


def attend_kernel(counts_ref, early_ref, late_ref, text_ref, out_ref, rows_ref, *, orders):
    tile = pl.program_id(0)
    patch = counts_ref[0, tile]
    texts = counts_ref[1, tile]
    mine = counts_ref[2, 0]
    length = patch + texts
    parts, local_rows, outs = rows_ref.shape
    for ref, order in zip((early_ref, late_ref), orders):
        for at, s in enumerate(order):
            rows_ref[lax.rem(mine + (parts - s), parts)] = ref[at, 0]
    rows = parts * local_rows
    row = lax.broadcasted_iota(jnp.int32, (rows, WINDOW), 0)
    place = lax.broadcasted_iota(jnp.int32, (rows, WINDOW), 1)
    placing = jnp.where((row == patch + place) & (place < texts), 1.0, 0.0).astype(jnp.bfloat16)
    placed = jnp.dot(placing, text_ref[...], preferred_element_type=jnp.float32)
    image_row = lax.broadcasted_iota(jnp.int32, (rows, outs), 0) < patch
    qkv = jnp.where(
        image_row, rows_ref[...].reshape(rows, outs).astype(jnp.float32), placed
    ).astype(jnp.bfloat16)
    keys = qkv[:, GROUP * HS : (GROUP + 1) * HS]
    values = qkv[:, (GROUP + 1) * HS :]
    at_row = lax.broadcasted_iota(jnp.int32, (rows, rows), 0)
    at_col = lax.broadcasted_iota(jnp.int32, (rows, rows), 1)
    allowed = (at_col <= at_row) & (at_col < length)
    for g in range(GROUP):
        scores = lax.dot_general(
            qkv[:, g * HS : (g + 1) * HS],
            keys,
            (((1,), (1,)), ((), ())),
            preferred_element_type=jnp.float32,
        ) * (1.0 / math.sqrt(HS))
        scores = jnp.where(allowed, scores, -1e30)
        row_max = jnp.max(scores, axis=1, keepdims=True)
        weights = jnp.where(allowed, jnp.exp(scores - row_max), 0.0)
        probabilities = (weights / jnp.sum(weights, axis=1, keepdims=True)).astype(jnp.bfloat16)
        attended = jnp.dot(probabilities, values, preferred_element_type=jnp.float32)
        out_ref[:, :, :, g * HS : (g + 1) * HS] = attended.astype(jnp.bfloat16).reshape(
            parts, 1, local_rows, HS
        )


def attend(early, late, orders, text_qkv, counts):
    tiles, local_rows, outs = early.shape[1:]
    parts = early.shape[0] + late.shape[0]
    rows = parts * local_rows
    return pl.pallas_call(
        functools.partial(attend_kernel, orders=orders),
        grid_spec=pltpu.PrefetchScalarGridSpec(
            num_scalar_prefetch=1,
            grid=(tiles,),
            in_specs=[
                pl.BlockSpec((early.shape[0], 1, local_rows, outs), lambda t, c: (0, t, 0, 0)),
                pl.BlockSpec((late.shape[0], 1, local_rows, outs), lambda t, c: (0, t, 0, 0)),
                pl.BlockSpec((WINDOW, outs), lambda t, c: (t, 0)),
            ],
            out_specs=pl.BlockSpec((parts, 1, local_rows, GROUP * HS), lambda t, c: (0, t, 0, 0)),
            scratch_shapes=[pltpu.VMEM((parts, local_rows, outs), jnp.bfloat16)],
        ),
        out_shape=jax.ShapeDtypeStruct((parts, tiles, local_rows, GROUP * HS), jnp.bfloat16),
        compiler_params=pltpu.CompilerParams(dimension_semantics=("arbitrary",)),
        cost_estimate=pl.CostEstimate(
            flops=tiles * rows * (2 * WINDOW * outs + 4 * GROUP * rows * HS),
            bytes_accessed=4 * tiles * rows * outs,
            transcendentals=tiles * GROUP * rows * rows,
        ),
    )(counts, early, late, text_qkv)


def out_kernel(att_ref, weight_ref, hidden_ref, out_ref, rows_ref):
    heads, _, head_width = att_ref.shape

    @pl.when(pl.program_id(0) == 0)
    def _():
        for h in range(heads):
            rows_ref[:, h * head_width : (h + 1) * head_width] = att_ref[h]

    weights = jnp.concatenate([weight_ref[j] for j in range(weight_ref.shape[0])], axis=1)
    total = jnp.dot(rows_ref[...], weights, preferred_element_type=jnp.float32)
    out_ref[...] = (hidden_ref[...].astype(jnp.float32) + total).astype(jnp.bfloat16)


def project_out(attended, weight_blocks, hidden):
    heads, rows, head_width = attended.shape
    blocks, depth, width = weight_blocks.shape
    step = 4
    return pl.pallas_call(
        out_kernel,
        grid=(blocks // step,),
        in_specs=[
            pl.BlockSpec((heads, rows, head_width), lambda i: (0, 0, 0)),
            pl.BlockSpec((step, depth, width), lambda i: (i, 0, 0)),
            pl.BlockSpec((rows, step * width), lambda i: (0, i)),
        ],
        out_specs=pl.BlockSpec((rows, step * width), lambda i: (0, i)),
        out_shape=jax.ShapeDtypeStruct((rows, blocks * width), jnp.bfloat16),
        scratch_shapes=[pltpu.VMEM((rows, depth), jnp.bfloat16)],
        compiler_params=pltpu.CompilerParams(dimension_semantics=("arbitrary",)),
        cost_estimate=pl.CostEstimate(
            flops=2 * rows * depth * blocks * width,
            bytes_accessed=2 * depth * blocks * width,
            transcendentals=0,
        ),
    )(attended, weight_blocks, hidden)


def body(
    vit_features,
    patch_counts,
    text_counts,
    tile_dest,
    text_embeds,
    w_proj,
    b_proj,
    norm_gain,
    w_qkv,
    w_out,
):
    parts = lax.axis_size("mp")
    mine = lax.axis_index("mp")
    image_count, local_rows, _ = vit_features.shape
    model_width = text_embeds.shape[-1]
    slice_width = model_width // parts
    each = image_count * local_rows
    lengths = patch_counts + text_counts
    counts = jnp.stack([patch_counts, text_counts, jnp.full((image_count,), mine, jnp.int32)])

    all_qkv = lax.all_gather(w_qkv[0, :, 0], "dp", axis=0, tiled=True)

    payload = pack(text_embeds, w_out[0, 0], mine, parts)
    got = [payload[0]] + [shifted(payload[s], "mp", s) for s in range(1, parts)]
    window, all_heads = unpack(got, counts, image_count, slice_width, w_out.shape[3])
    all_out = lax.all_gather(all_heads[None], "dp", axis=0, tiled=True)

    arrived = exchange_tiles(vit_features, tile_dest)
    chunks = ring_chunks(arrived, "mp")
    text_chunks = ring_chunks(window, "mp")

    text_places = patch_counts[:, None] + jnp.arange(WINDOW, dtype=jnp.int32)[None, :]
    text_cos, text_sin = rotation_tables(text_places.reshape(-1))
    half = parts // 2
    near = [0] + [s for k in range(1, half - 1) for s in (k, parts - k)]
    far = [half - 1, half + 1, half]
    orders = (tuple(near), tuple(far))
    local = jnp.arange(local_rows, dtype=jnp.int32)
    begins = jnp.stack([lax.rem(mine + (parts - s), parts) * local_rows for s in near + far])
    chunk_cos, chunk_sin = rotation_tables(begins[:, None] + local[None, :])

    bias = b_proj.reshape(1, model_width)
    early, own_projected = image_qkv_of(
        [chunks[s] for s in near],
        chunk_cos[: len(near)],
        chunk_sin[: len(near)],
        w_proj,
        bias,
        norm_gain,
        all_qkv,
        True,
    )
    (late,) = image_qkv_of(
        [chunks[s] for s in far],
        chunk_cos[len(near) :],
        chunk_sin[len(near) :],
        w_proj,
        bias,
        norm_gain,
        all_qkv,
        False,
    )
    text_qkv = text_qkv_of(text_chunks, mine, text_cos, text_sin, norm_gain, all_qkv)

    own_rows = (mine * local_rows + local)[None, :, None]
    hidden = jnp.where(
        own_rows < patch_counts[:, None, None],
        own_projected.reshape(image_count, local_rows, model_width),
        jnp.where(
            own_rows < lengths[:, None, None], text_embeds, jnp.zeros_like(text_embeds)
        ),
    ).reshape(each, model_width)

    attended = attend(early, late, orders, text_qkv, counts)
    returned = lax.all_to_all(
        attended.reshape(parts, each, -1), "mp", split_axis=0, concat_axis=0, tiled=True
    )
    out = project_out(returned, all_out, hidden)
    return out.reshape(image_count, local_rows, model_width)


def solution(mesh):
    in_specs = (
        P("dp", "mp", None),
        P("dp"),
        P("dp"),
        P("dp"),
        P("dp", "mp", None),
        P(),
        P(),
        P(),
        P(None, "dp", "mp", None),
        P(None, "mp", None, "dp"),
    )
    out_specs = P("dp", "mp", None)

    return jax.shard_map(body, mesh=mesh, in_specs=in_specs, out_specs=out_specs, check_vma=False)
```

```python
import functools
import math

import jax
import jax.numpy as jnp
from jax import lax
from jax.experimental import pallas as pl
from jax.experimental.pallas import tpu as pltpu
from jax.sharding import PartitionSpec as P


HS = 128
GROUP = 2
WINDOW = 64
IMAGE_ROWS = 192
EXTRA = 128

rope_base = 500000.0
epsilon = 1e-05


def shifted(value, axis, step, sources=None):
    size = lax.axis_size(axis)
    pairs = [(i, (i + step) % size) for i in range(size) if sources is None or i in sources]
    return lax.ppermute(value, axis, pairs)


def ring_chunks(own, axis, useful=None):
    size = lax.axis_size(axis)
    useful = size if useful is None else useful
    chunks = [own] + [None] * (size - 1)
    for s in range(1, size // 2 + 1):
        holders = [(o + s - 1) % size for o in range(useful)]
        chunks[s] = shifted(chunks[s - 1], axis, 1, holders)
        if s < size - s:
            holders = [(o - s + 1) % size for o in range(useful)]
            chunks[size - s] = shifted(chunks[(size - s + 1) % size], axis, -1, holders)
    return chunks


def rotation_tables(rows):
    half_size = HS // 2
    inverse = jnp.exp(
        -(2.0 * jnp.arange(half_size, dtype=jnp.float32) / HS) * math.log(rope_base)
    )
    angles = rows.astype(jnp.float32)[..., None] * inverse
    cosine, sine = jnp.cos(angles), jnp.sin(angles)
    return (
        jnp.concatenate([cosine, cosine], axis=-1),
        jnp.concatenate([-sine, sine], axis=-1),
    )


def rotate_store(joined, cosine, sine, store):
    heads = joined.shape[1] // HS
    for p in range(heads):
        part = joined[:, p * HS : (p + 1) * HS]
        if p < heads - 1:
            part = part * cosine + pltpu.roll(part, HS // 2, 1) * sine
        store(p, part.astype(jnp.bfloat16))


def order_kernel(got_ref, out_ref, *, image_count):
    total, wide = got_ref.shape
    width = wide - EXTRA
    dest = got_ref[:, width:].astype(jnp.float32)
    row = lax.broadcasted_iota(jnp.int32, (total, total), 0)
    col = lax.broadcasted_iota(jnp.int32, (total, total), 1)
    earlier = (dest == dest.T) & (col < row)
    slots = jnp.sum(jnp.where(earlier, 1.0, 0.0), axis=1, keepdims=True)
    targets = (dest * image_count + slots).T
    placing = jnp.where(targets == row.astype(jnp.float32), 1.0, 0.0).astype(jnp.bfloat16)
    out_ref[...] = jnp.dot(
        placing, got_ref[:, :width], preferred_element_type=jnp.float32
    ).astype(jnp.bfloat16)


def exchange_tiles(vit_features, tile_dest):
    image_count, _, width = vit_features.shape
    ranks = lax.axis_size("dp")
    by_row = jnp.moveaxis(vit_features, 1, 0)
    tags = jnp.broadcast_to(
        tile_dest.astype(jnp.bfloat16)[None, :, None], (ranks, image_count, EXTRA)
    )
    sent = jnp.concatenate([by_row, tags], axis=2)
    got = lax.all_to_all(sent, "dp", split_axis=0, concat_axis=0, tiled=True)
    total = ranks * image_count
    ordered = pl.pallas_call(
        functools.partial(order_kernel, image_count=image_count),
        out_shape=jax.ShapeDtypeStruct((total, width), jnp.bfloat16),
        cost_estimate=pl.CostEstimate(
            flops=2 * total * total * width, bytes_accessed=4 * total * width, transcendentals=0
        ),
    )(got.reshape(total, width + EXTRA))
    arrived = lax.all_to_all(
        ordered.reshape(ranks, image_count, width),
        "dp",
        split_axis=0,
        concat_axis=0,
        tiled=True,
    )
    return jnp.moveaxis(arrived, 0, 1)


def pack_kernel(place_ref, text_ref, heads_ref, *out_refs):
    parts = len(out_refs)
    rows, wide = out_refs[0].shape
    folds = heads_ref.shape[0] // rows
    cols = heads_ref.shape[1]
    width = wide - folds * cols
    mine = place_ref[0]
    for s, out_ref in enumerate(out_refs):
        at = pl.multiple_of(lax.rem(mine + s, parts) * width, width)
        out_ref[:, :width] = text_ref[:, :, pl.ds(at, width)].reshape(rows, width)
        for f in range(folds):
            out_ref[:, width + f * cols : width + (f + 1) * cols] = heads_ref[
                f * rows : (f + 1) * rows, :
            ]


def pack(text_embeds, head_rows, mine, parts):
    tiles, local_rows, model_width = text_embeds.shape
    rows = tiles * local_rows
    width = model_width // parts
    wide = width + head_rows.shape[0] * head_rows.shape[1] // rows
    whole = pl.BlockSpec(memory_space=pltpu.VMEM)
    return pl.pallas_call(
        pack_kernel,
        in_specs=[pl.BlockSpec(memory_space=pltpu.SMEM), whole, whole],
        out_specs=[whole] * parts,
        out_shape=[jax.ShapeDtypeStruct((rows, wide), jnp.bfloat16)] * parts,
        cost_estimate=pl.CostEstimate(
            flops=1 << 20, bytes_accessed=4 * parts * rows * wide, transcendentals=0
        ),
    )(mine.reshape(1), text_embeds, head_rows)


def unpack_kernel(counts_ref, *refs, tiles, width):
    parts = len(refs) - 3
    got_refs = refs[:parts]
    window_ref, heads_ref, rows_ref = refs[parts:]
    mine = counts_ref[2, 0]
    each, wide = got_refs[0].shape
    local_rows = each // tiles
    cols = heads_ref.shape[1]
    folds = (wide - width) // cols
    for s, got_ref in enumerate(got_refs):
        at = lax.rem(mine + (parts - s), parts)
        for f in range(folds):
            begin = pl.multiple_of((at * folds + f) * each, each)
            heads_ref[pl.ds(begin, each), :] = got_ref[:, width + f * cols : width + (f + 1) * cols]
        for t in range(tiles):
            rows_ref[t, at] = got_ref[t * local_rows : (t + 1) * local_rows, :width]
    rows = parts * local_rows
    place = lax.broadcasted_iota(jnp.int32, (WINDOW, rows), 0)
    row = lax.broadcasted_iota(jnp.int32, (WINDOW, rows), 1)
    for t in range(tiles):
        picks = (row == counts_ref[0, t] + place) & (place < counts_ref[1, t])
        window_ref[t * WINDOW : (t + 1) * WINDOW, :] = jnp.dot(
            jnp.where(picks, 1.0, 0.0).astype(jnp.bfloat16),
            rows_ref[t].reshape(rows, width),
            preferred_element_type=jnp.float32,
        ).astype(jnp.bfloat16)


def unpack(got, counts, tiles, width, cols):
    parts = len(got)
    each, wide = got[0].shape
    local_rows = each // tiles
    whole = pl.BlockSpec(memory_space=pltpu.VMEM)
    return pl.pallas_call(
        functools.partial(unpack_kernel, tiles=tiles, width=width),
        in_specs=[pl.BlockSpec(memory_space=pltpu.SMEM)] + [whole] * parts,
        out_specs=[whole, whole],
        out_shape=[
            jax.ShapeDtypeStruct((tiles * WINDOW, width), jnp.bfloat16),
            jax.ShapeDtypeStruct((parts * each * ((wide - width) // cols), cols), jnp.bfloat16),
        ],
        scratch_shapes=[pltpu.VMEM((tiles, parts, local_rows, width), jnp.bfloat16)],
        cost_estimate=pl.CostEstimate(
            flops=2 * tiles * WINDOW * parts * local_rows * width,
            bytes_accessed=2 * parts * each * wide,
            transcendentals=0,
        ),
    )(counts, *got)


def text_kernel(place_ref, *refs):
    parts = len(refs) - 5
    chunk_refs = refs[:parts]
    cos_ref, sin_ref, gain_ref, weight_ref, out_ref = refs[parts:]
    width = chunk_refs[0].shape[1]
    mine = place_ref[0]
    squares = None
    total = None
    for s, chunk_ref in enumerate(chunk_refs):
        at = lax.rem(mine + (parts - s), parts)
        rows = chunk_ref[...].astype(jnp.float32)
        part = jnp.sum(rows * rows, axis=1, keepdims=True)
        squares = part if squares is None else squares + part
        scaled = (rows * gain_ref[pl.ds(at, 1), :]).astype(jnp.bfloat16)
        block = weight_ref[pl.ds(pl.multiple_of(at * width, width), width), :]
        term = jnp.dot(scaled, block, preferred_element_type=jnp.float32)
        total = term if total is None else total + term
    scale = lax.rsqrt(squares * (1.0 / (parts * width)) + epsilon)

    def store(p, value):
        out_ref[:, p * HS : (p + 1) * HS] = value

    rotate_store(total * scale, cos_ref[...], sin_ref[...], store)


def text_qkv_of(chunks, mine, cosine, sine, gain, all_qkv):
    rows, width = chunks[0].shape
    parts = len(chunks)
    outs = all_qkv.shape[1]
    whole = pl.BlockSpec(memory_space=pltpu.VMEM)
    return pl.pallas_call(
        text_kernel,
        in_specs=[pl.BlockSpec(memory_space=pltpu.SMEM)] + [whole] * (parts + 4),
        out_specs=whole,
        out_shape=jax.ShapeDtypeStruct((rows, outs), jnp.bfloat16),
        cost_estimate=pl.CostEstimate(
            flops=2 * rows * parts * width * outs,
            bytes_accessed=2 * parts * width * (rows + outs),
            transcendentals=0,
        ),
    )(mine.reshape(1), *chunks, cosine, sine, gain.reshape(parts, width), all_qkv)


def image_kernel(*refs, groups, with_hidden):
    chunk_refs = refs[:groups]
    cos_ref, sin_ref, proj_ref, bias_ref, gain_ref, qkv_ref = refs[groups : groups + 6]
    out_ref = refs[groups + 6]
    hidden_ref = refs[groups + 7] if with_hidden else None
    rows_ref, sum_ref, squares_ref = refs[-3:]
    tiles, local_rows, depth = chunk_refs[0].shape
    each = tiles * local_rows
    step = pl.program_id(0)

    @pl.when(step == 0)
    def _():
        for g, chunk_ref in enumerate(chunk_refs):
            rows_ref[g * each : (g + 1) * each, :] = chunk_ref[...].reshape(each, depth)
        sum_ref[...] = jnp.zeros_like(sum_ref)
        squares_ref[...] = jnp.zeros_like(squares_ref)

    projected = (
        jnp.dot(rows_ref[...], proj_ref[...], preferred_element_type=jnp.float32) + bias_ref[...]
    ).astype(jnp.bfloat16)
    if with_hidden:
        hidden_ref[...] = projected[:each]
    wide = projected.astype(jnp.float32)
    squares_ref[...] += jnp.sum(wide * wide, axis=1, keepdims=True)
    scaled = (wide * gain_ref[...]).astype(jnp.bfloat16)
    sum_ref[...] += jnp.dot(scaled, qkv_ref[...], preferred_element_type=jnp.float32)

    @pl.when(step == pl.num_programs(0) - 1)
    def _():
        model_width = proj_ref.shape[1] * pl.num_programs(0)
        scale = lax.rsqrt(squares_ref[...] * (1.0 / model_width) + epsilon)
        shape = (groups, tiles, local_rows, HS)
        cosine = jnp.broadcast_to(cos_ref[...][:, None], shape).reshape(groups * each, HS)
        sine = jnp.broadcast_to(sin_ref[...][:, None], shape).reshape(groups * each, HS)

        def store(p, value):
            out_ref[:, :, :, p * HS : (p + 1) * HS] = value.reshape(shape)

        rotate_store(sum_ref[...] * scale, cosine, sine, store)


def image_qkv_of(chunks, cosine, sine, w_proj, bias, gain, all_qkv, with_hidden):
    groups = len(chunks)
    tiles, local_rows, depth = chunks[0].shape
    model_width, outs = all_qkv.shape
    each = tiles * local_rows
    block = 512
    fixed = lambda *shape: pl.BlockSpec(shape, lambda i: (0,) * len(shape))
    out_specs = [fixed(groups, tiles, local_rows, outs)]
    out_shape = [jax.ShapeDtypeStruct((groups, tiles, local_rows, outs), jnp.bfloat16)]
    if with_hidden:
        out_specs.append(pl.BlockSpec((each, block), lambda i: (0, i)))
        out_shape.append(jax.ShapeDtypeStruct((each, model_width), jnp.bfloat16))
    return pl.pallas_call(
        functools.partial(image_kernel, groups=groups, with_hidden=with_hidden),
        grid=(model_width // block,),
        in_specs=[fixed(tiles, local_rows, depth)] * groups
        + [
            fixed(groups, local_rows, HS),
            fixed(groups, local_rows, HS),
            pl.BlockSpec((depth, block), lambda i: (0, i)),
            pl.BlockSpec((1, block), lambda i: (0, i)),
            pl.BlockSpec((1, block), lambda i: (0, i)),
            pl.BlockSpec((block, outs), lambda i: (i, 0)),
        ],
        out_specs=out_specs,
        out_shape=out_shape,
        scratch_shapes=[
            pltpu.VMEM((groups * each, depth), jnp.bfloat16),
            pltpu.VMEM((groups * each, outs), jnp.float32),
            pltpu.VMEM((groups * each, 1), jnp.float32),
        ],
        compiler_params=pltpu.CompilerParams(dimension_semantics=("arbitrary",)),
        cost_estimate=pl.CostEstimate(
            flops=2 * groups * each * model_width * (depth + outs),
            bytes_accessed=2 * model_width * (depth + outs),
            transcendentals=0,
        ),
    )(*chunks, cosine, sine, w_proj, bias, gain, all_qkv)


def attend_kernel(counts_ref, early_ref, late_ref, text_ref, out_ref, rows_ref, *, orders):
    tile = pl.program_id(0)
    patch = counts_ref[0, tile]
    texts = counts_ref[1, tile]
    mine = counts_ref[2, 0]
    length = patch + texts
    parts, local_rows, outs = rows_ref.shape
    for ref, order in zip((early_ref, late_ref), orders):
        for at, s in enumerate(order):
            rows_ref[lax.rem(mine + (parts - s), parts)] = ref[at, 0]
    rows = parts * local_rows
    row = lax.broadcasted_iota(jnp.int32, (rows, WINDOW), 0)
    place = lax.broadcasted_iota(jnp.int32, (rows, WINDOW), 1)
    placing = jnp.where((row == patch + place) & (place < texts), 1.0, 0.0).astype(jnp.bfloat16)
    placed = jnp.dot(placing, text_ref[...], preferred_element_type=jnp.float32)
    image_row = lax.broadcasted_iota(jnp.int32, (rows, outs), 0) < patch
    qkv = jnp.where(
        image_row, rows_ref[...].reshape(rows, outs).astype(jnp.float32), placed
    ).astype(jnp.bfloat16)
    keys = qkv[:, GROUP * HS : (GROUP + 1) * HS]
    values = qkv[:, (GROUP + 1) * HS :]
    at_row = lax.broadcasted_iota(jnp.int32, (rows, rows), 0)
    at_col = lax.broadcasted_iota(jnp.int32, (rows, rows), 1)
    allowed = (at_col <= at_row) & (at_col < length)
    for g in range(GROUP):
        scores = lax.dot_general(
            qkv[:, g * HS : (g + 1) * HS],
            keys,
            (((1,), (1,)), ((), ())),
            preferred_element_type=jnp.float32,
        ) * (1.0 / math.sqrt(HS))
        scores = jnp.where(allowed, scores, -1e30)
        row_max = jnp.max(scores, axis=1, keepdims=True)
        weights = jnp.where(allowed, jnp.exp(scores - row_max), 0.0)
        probabilities = (weights / jnp.sum(weights, axis=1, keepdims=True)).astype(jnp.bfloat16)
        attended = jnp.dot(probabilities, values, preferred_element_type=jnp.float32)
        out_ref[:, :, :, g * HS : (g + 1) * HS] = attended.astype(jnp.bfloat16).reshape(
            parts, 1, local_rows, HS
        )


def attend(early, late, orders, text_qkv, counts):
    tiles, local_rows, outs = early.shape[1:]
    parts = early.shape[0] + late.shape[0]
    rows = parts * local_rows
    return pl.pallas_call(
        functools.partial(attend_kernel, orders=orders),
        grid_spec=pltpu.PrefetchScalarGridSpec(
            num_scalar_prefetch=1,
            grid=(tiles,),
            in_specs=[
                pl.BlockSpec((early.shape[0], 1, local_rows, outs), lambda t, c: (0, t, 0, 0)),
                pl.BlockSpec((late.shape[0], 1, local_rows, outs), lambda t, c: (0, t, 0, 0)),
                pl.BlockSpec((WINDOW, outs), lambda t, c: (t, 0)),
            ],
            out_specs=pl.BlockSpec((parts, 1, local_rows, GROUP * HS), lambda t, c: (0, t, 0, 0)),
            scratch_shapes=[pltpu.VMEM((parts, local_rows, outs), jnp.bfloat16)],
        ),
        out_shape=jax.ShapeDtypeStruct((parts, tiles, local_rows, GROUP * HS), jnp.bfloat16),
        compiler_params=pltpu.CompilerParams(dimension_semantics=("arbitrary",)),
        cost_estimate=pl.CostEstimate(
            flops=tiles * rows * (2 * WINDOW * outs + 4 * GROUP * rows * HS),
            bytes_accessed=4 * tiles * rows * outs,
            transcendentals=tiles * GROUP * rows * rows,
        ),
    )(counts, early, late, text_qkv)


def out_kernel(att_ref, weight_ref, hidden_ref, out_ref, rows_ref):
    heads, _, head_width = att_ref.shape

    @pl.when(pl.program_id(0) == 0)
    def _():
        for h in range(heads):
            rows_ref[:, h * head_width : (h + 1) * head_width] = att_ref[h]

    weights = jnp.concatenate([weight_ref[j] for j in range(weight_ref.shape[0])], axis=1)
    total = jnp.dot(rows_ref[...], weights, preferred_element_type=jnp.float32)
    out_ref[...] = (hidden_ref[...].astype(jnp.float32) + total).astype(jnp.bfloat16)


def project_out(attended, weight_blocks, hidden):
    heads, rows, head_width = attended.shape
    blocks, depth, width = weight_blocks.shape
    step = 4
    return pl.pallas_call(
        out_kernel,
        grid=(blocks // step,),
        in_specs=[
            pl.BlockSpec((heads, rows, head_width), lambda i: (0, 0, 0)),
            pl.BlockSpec((step, depth, width), lambda i: (i, 0, 0)),
            pl.BlockSpec((rows, step * width), lambda i: (0, i)),
        ],
        out_specs=pl.BlockSpec((rows, step * width), lambda i: (0, i)),
        out_shape=jax.ShapeDtypeStruct((rows, blocks * width), jnp.bfloat16),
        scratch_shapes=[pltpu.VMEM((rows, depth), jnp.bfloat16)],
        compiler_params=pltpu.CompilerParams(dimension_semantics=("arbitrary",)),
        cost_estimate=pl.CostEstimate(
            flops=2 * rows * depth * blocks * width,
            bytes_accessed=2 * depth * blocks * width,
            transcendentals=0,
        ),
    )(attended, weight_blocks, hidden)


def body(
    vit_features,
    patch_counts,
    text_counts,
    tile_dest,
    text_embeds,
    w_proj,
    b_proj,
    norm_gain,
    w_qkv,
    w_out,
):
    parts = lax.axis_size("mp")
    mine = lax.axis_index("mp")
    image_count, local_rows, _ = vit_features.shape
    model_width = text_embeds.shape[-1]
    slice_width = model_width // parts
    each = image_count * local_rows
    lengths = patch_counts + text_counts
    counts = jnp.stack([patch_counts, text_counts, jnp.full((image_count,), mine, jnp.int32)])

    all_qkv = lax.all_gather(w_qkv[0, :, 0], "dp", axis=0, tiled=True)

    payload = pack(text_embeds, w_out[0, 0], mine, parts)
    got = [payload[0]] + [shifted(payload[s], "mp", s) for s in range(1, parts)]
    window, all_heads = unpack(got, counts, image_count, slice_width, w_out.shape[3])
    all_out = lax.all_gather(all_heads[None], "dp", axis=0, tiled=True)

    arrived = exchange_tiles(vit_features, tile_dest)
    chunks = ring_chunks(arrived, "mp", -(-IMAGE_ROWS // local_rows))
    text_chunks = ring_chunks(window, "mp")

    text_places = patch_counts[:, None] + jnp.arange(WINDOW, dtype=jnp.int32)[None, :]
    text_cos, text_sin = rotation_tables(text_places.reshape(-1))
    half = parts // 2
    near = [0] + [s for k in range(1, half - 1) for s in (k, parts - k)]
    far = [half - 1, half + 1, half]
    orders = (tuple(near), tuple(far))
    local = jnp.arange(local_rows, dtype=jnp.int32)
    begins = jnp.stack([lax.rem(mine + (parts - s), parts) * local_rows for s in near + far])
    chunk_cos, chunk_sin = rotation_tables(begins[:, None] + local[None, :])

    bias = b_proj.reshape(1, model_width)
    early, own_projected = image_qkv_of(
        [chunks[s] for s in near],
        chunk_cos[: len(near)],
        chunk_sin[: len(near)],
        w_proj,
        bias,
        norm_gain,
        all_qkv,
        True,
    )
    (late,) = image_qkv_of(
        [chunks[s] for s in far],
        chunk_cos[len(near) :],
        chunk_sin[len(near) :],
        w_proj,
        bias,
        norm_gain,
        all_qkv,
        False,
    )
    text_qkv = text_qkv_of(text_chunks, mine, text_cos, text_sin, norm_gain, all_qkv)

    own_rows = (mine * local_rows + local)[None, :, None]
    hidden = jnp.where(
        own_rows < patch_counts[:, None, None],
        own_projected.reshape(image_count, local_rows, model_width),
        jnp.where(
            own_rows < lengths[:, None, None], text_embeds, jnp.zeros_like(text_embeds)
        ),
    ).reshape(each, model_width)

    attended = attend(early, late, orders, text_qkv, counts)
    returned = lax.all_to_all(
        attended.reshape(parts, each, -1), "mp", split_axis=0, concat_axis=0, tiled=True
    )
    out = project_out(returned, all_out, hidden)
    return out.reshape(image_count, local_rows, model_width)


def solution(mesh):
    in_specs = (
        P("dp", "mp", None),
        P("dp"),
        P("dp"),
        P("dp"),
        P("dp", "mp", None),
        P(),
        P(),
        P(),
        P(None, "dp", "mp", None),
        P(None, "mp", None, "dp"),
    )
    out_specs = P("dp", "mp", None)

    return jax.shard_map(body, mesh=mesh, in_specs=in_specs, out_specs=out_specs, check_vma=False)
```

```python
import functools
import math

import jax
import jax.numpy as jnp
from jax import lax
from jax.experimental import pallas as pl
from jax.experimental.pallas import tpu as pltpu
from jax.sharding import PartitionSpec as P


HS = 128
GROUP = 2
WINDOW = 64
IMAGE_ROWS = 192
EXTRA = 128

rope_base = 500000.0
epsilon = 1e-05


def shifted(value, axis, step, sources=None):
    size = lax.axis_size(axis)
    pairs = [(i, (i + step) % size) for i in range(size) if sources is None or i in sources]
    return lax.ppermute(value, axis, pairs)


def ring_chunks(own, axis, useful=None):
    size = lax.axis_size(axis)
    useful = size if useful is None else useful
    chunks = [own] + [None] * (size - 1)
    for s in range(1, size // 2 + 1):
        holders = [(o + s - 1) % size for o in range(useful)]
        chunks[s] = shifted(chunks[s - 1], axis, 1, holders)
        if s < size - s:
            holders = [(o - s + 1) % size for o in range(useful)]
            chunks[size - s] = shifted(chunks[(size - s + 1) % size], axis, -1, holders)
    return chunks


def rotation_tables(rows):
    half_size = HS // 2
    inverse = jnp.exp(
        -(2.0 * jnp.arange(half_size, dtype=jnp.float32) / HS) * math.log(rope_base)
    )
    angles = rows.astype(jnp.float32)[..., None] * inverse
    cosine, sine = jnp.cos(angles), jnp.sin(angles)
    return (
        jnp.concatenate([cosine, cosine], axis=-1),
        jnp.concatenate([-sine, sine], axis=-1),
    )


def rotate_store(joined, cosine, sine, store):
    heads = joined.shape[1] // HS
    for p in range(heads):
        part = joined[:, p * HS : (p + 1) * HS]
        if p < heads - 1:
            part = part * cosine + pltpu.roll(part, HS // 2, 1) * sine
        store(p, part.astype(jnp.bfloat16))


def order_kernel(got_ref, out_ref, *, image_count):
    total, wide = got_ref.shape
    width = wide - EXTRA
    dest = got_ref[:, width:].astype(jnp.float32)
    row = lax.broadcasted_iota(jnp.int32, (total, total), 0)
    col = lax.broadcasted_iota(jnp.int32, (total, total), 1)
    earlier = (dest == dest.T) & (col < row)
    slots = jnp.sum(jnp.where(earlier, 1.0, 0.0), axis=1, keepdims=True)
    targets = (dest * image_count + slots).T
    placing = jnp.where(targets == row.astype(jnp.float32), 1.0, 0.0).astype(jnp.bfloat16)
    out_ref[...] = jnp.dot(
        placing, got_ref[:, :width], preferred_element_type=jnp.float32
    ).astype(jnp.bfloat16)


def exchange_tiles(vit_features, tile_dest):
    image_count, _, width = vit_features.shape
    ranks = lax.axis_size("dp")
    by_row = jnp.moveaxis(vit_features, 1, 0)
    tags = jnp.broadcast_to(
        tile_dest.astype(jnp.bfloat16)[None, :, None], (ranks, image_count, EXTRA)
    )
    sent = jnp.concatenate([by_row, tags], axis=2)
    got = lax.all_to_all(sent, "dp", split_axis=0, concat_axis=0, tiled=True)
    total = ranks * image_count
    ordered = pl.pallas_call(
        functools.partial(order_kernel, image_count=image_count),
        out_shape=jax.ShapeDtypeStruct((total, width), jnp.bfloat16),
        cost_estimate=pl.CostEstimate(
            flops=2 * total * total * width, bytes_accessed=4 * total * width, transcendentals=0
        ),
    )(got.reshape(total, width + EXTRA))
    arrived = lax.all_to_all(
        ordered.reshape(ranks, image_count, width),
        "dp",
        split_axis=0,
        concat_axis=0,
        tiled=True,
    )
    return jnp.moveaxis(arrived, 0, 1)


def pack_kernel(place_ref, text_ref, heads_ref, *out_refs):
    parts = len(out_refs)
    rows, wide = out_refs[0].shape
    folds = heads_ref.shape[0] // rows
    cols = heads_ref.shape[1]
    width = wide - folds * cols
    mine = place_ref[0]
    for s, out_ref in enumerate(out_refs):
        at = pl.multiple_of(lax.rem(mine + s, parts) * width, width)
        out_ref[:, :width] = text_ref[:, :, pl.ds(at, width)].reshape(rows, width)
        for f in range(folds):
            out_ref[:, width + f * cols : width + (f + 1) * cols] = heads_ref[
                f * rows : (f + 1) * rows, :
            ]


def pack(text_embeds, head_rows, mine, parts):
    tiles, local_rows, model_width = text_embeds.shape
    rows = tiles * local_rows
    width = model_width // parts
    wide = width + head_rows.shape[0] * head_rows.shape[1] // rows
    whole = pl.BlockSpec(memory_space=pltpu.VMEM)
    return pl.pallas_call(
        pack_kernel,
        in_specs=[pl.BlockSpec(memory_space=pltpu.SMEM), whole, whole],
        out_specs=[whole] * parts,
        out_shape=[jax.ShapeDtypeStruct((rows, wide), jnp.bfloat16)] * parts,
        cost_estimate=pl.CostEstimate(
            flops=1 << 20, bytes_accessed=4 * parts * rows * wide, transcendentals=0
        ),
    )(mine.reshape(1), text_embeds, head_rows)


def unpack_kernel(counts_ref, *refs, tiles, width):
    parts = len(refs) - 3
    got_refs = refs[:parts]
    window_ref, heads_ref, rows_ref = refs[parts:]
    mine = counts_ref[2, 0]
    each, wide = got_refs[0].shape
    local_rows = each // tiles
    cols = heads_ref.shape[1]
    folds = (wide - width) // cols
    for s, got_ref in enumerate(got_refs):
        at = lax.rem(mine + (parts - s), parts)
        for f in range(folds):
            begin = pl.multiple_of((at * folds + f) * each, each)
            heads_ref[pl.ds(begin, each), :] = got_ref[:, width + f * cols : width + (f + 1) * cols]
        for t in range(tiles):
            rows_ref[t, at] = got_ref[t * local_rows : (t + 1) * local_rows, :width]
    rows = parts * local_rows
    place = lax.broadcasted_iota(jnp.int32, (WINDOW, rows), 0)
    row = lax.broadcasted_iota(jnp.int32, (WINDOW, rows), 1)
    for t in range(tiles):
        picks = (row == counts_ref[0, t] + place) & (place < counts_ref[1, t])
        window_ref[t * WINDOW : (t + 1) * WINDOW, :] = jnp.dot(
            jnp.where(picks, 1.0, 0.0).astype(jnp.bfloat16),
            rows_ref[t].reshape(rows, width),
            preferred_element_type=jnp.float32,
        ).astype(jnp.bfloat16)


def unpack(got, counts, tiles, width, cols):
    parts = len(got)
    each, wide = got[0].shape
    local_rows = each // tiles
    whole = pl.BlockSpec(memory_space=pltpu.VMEM)
    return pl.pallas_call(
        functools.partial(unpack_kernel, tiles=tiles, width=width),
        in_specs=[pl.BlockSpec(memory_space=pltpu.SMEM)] + [whole] * parts,
        out_specs=[whole, whole],
        out_shape=[
            jax.ShapeDtypeStruct((tiles * WINDOW, width), jnp.bfloat16),
            jax.ShapeDtypeStruct((parts * each * ((wide - width) // cols), cols), jnp.bfloat16),
        ],
        scratch_shapes=[pltpu.VMEM((tiles, parts, local_rows, width), jnp.bfloat16)],
        cost_estimate=pl.CostEstimate(
            flops=2 * tiles * WINDOW * parts * local_rows * width,
            bytes_accessed=2 * parts * each * wide,
            transcendentals=0,
        ),
    )(counts, *got)


def text_kernel(place_ref, *refs):
    parts = len(refs) - 5
    chunk_refs = refs[:parts]
    cos_ref, sin_ref, gain_ref, weight_ref, out_ref = refs[parts:]
    width = chunk_refs[0].shape[1]
    mine = place_ref[0]
    squares = None
    total = None
    for s, chunk_ref in enumerate(chunk_refs):
        at = lax.rem(mine + (parts - s), parts)
        rows = chunk_ref[...].astype(jnp.float32)
        part = jnp.sum(rows * rows, axis=1, keepdims=True)
        squares = part if squares is None else squares + part
        scaled = (rows * gain_ref[pl.ds(at, 1), :]).astype(jnp.bfloat16)
        block = weight_ref[pl.ds(pl.multiple_of(at * width, width), width), :]
        term = jnp.dot(scaled, block, preferred_element_type=jnp.float32)
        total = term if total is None else total + term
    scale = lax.rsqrt(squares * (1.0 / (parts * width)) + epsilon)

    def store(p, value):
        out_ref[:, p * HS : (p + 1) * HS] = value

    rotate_store(total * scale, cos_ref[...], sin_ref[...], store)


def text_qkv_of(chunks, mine, cosine, sine, gain, all_qkv):
    rows, width = chunks[0].shape
    parts = len(chunks)
    outs = all_qkv.shape[1]
    whole = pl.BlockSpec(memory_space=pltpu.VMEM)
    return pl.pallas_call(
        text_kernel,
        in_specs=[pl.BlockSpec(memory_space=pltpu.SMEM)] + [whole] * (parts + 4),
        out_specs=whole,
        out_shape=jax.ShapeDtypeStruct((rows, outs), jnp.bfloat16),
        cost_estimate=pl.CostEstimate(
            flops=2 * rows * parts * width * outs,
            bytes_accessed=2 * parts * width * (rows + outs),
            transcendentals=0,
        ),
    )(mine.reshape(1), *chunks, cosine, sine, gain.reshape(parts, width), all_qkv)


def image_kernel(*refs, groups):
    chunk_refs = refs[:groups]
    cos_ref, sin_ref, proj_ref, bias_ref, gain_ref, qkv_ref = refs[groups : groups + 6]
    out_ref, hidden_ref, rows_ref, sum_ref, squares_ref = refs[groups + 6 :]
    tiles, local_rows, depth = chunk_refs[0].shape
    each = tiles * local_rows
    step = pl.program_id(0)

    @pl.when(step == 0)
    def _():
        for g, chunk_ref in enumerate(chunk_refs):
            rows_ref[g * each : (g + 1) * each, :] = chunk_ref[...].reshape(each, depth)
        sum_ref[...] = jnp.zeros_like(sum_ref)
        squares_ref[...] = jnp.zeros_like(squares_ref)

    projected = (
        jnp.dot(rows_ref[...], proj_ref[...], preferred_element_type=jnp.float32) + bias_ref[...]
    ).astype(jnp.bfloat16)
    hidden_ref[...] = projected[:each]
    wide = projected.astype(jnp.float32)
    squares_ref[...] += jnp.sum(wide * wide, axis=1, keepdims=True)
    scaled = (wide * gain_ref[...]).astype(jnp.bfloat16)
    sum_ref[...] += jnp.dot(scaled, qkv_ref[...], preferred_element_type=jnp.float32)

    @pl.when(step == pl.num_programs(0) - 1)
    def _():
        model_width = proj_ref.shape[1] * pl.num_programs(0)
        scale = lax.rsqrt(squares_ref[...] * (1.0 / model_width) + epsilon)
        shape = (groups, tiles, local_rows, HS)
        cosine = jnp.broadcast_to(cos_ref[...][:, None], shape).reshape(groups * each, HS)
        sine = jnp.broadcast_to(sin_ref[...][:, None], shape).reshape(groups * each, HS)

        def store(p, value):
            out_ref[:, :, :, p * HS : (p + 1) * HS] = value.reshape(shape)

        rotate_store(sum_ref[...] * scale, cosine, sine, store)


def image_qkv_of(chunks, cosine, sine, w_proj, bias, gain, all_qkv):
    groups = len(chunks)
    tiles, local_rows, depth = chunks[0].shape
    model_width, outs = all_qkv.shape
    each = tiles * local_rows
    block = 1024
    fixed = lambda *shape: pl.BlockSpec(shape, lambda i: (0,) * len(shape))
    out_specs = [
        fixed(groups, tiles, local_rows, outs),
        pl.BlockSpec((each, block), lambda i: (0, i)),
    ]
    out_shape = [
        jax.ShapeDtypeStruct((groups, tiles, local_rows, outs), jnp.bfloat16),
        jax.ShapeDtypeStruct((each, model_width), jnp.bfloat16),
    ]
    return pl.pallas_call(
        functools.partial(image_kernel, groups=groups),
        grid=(model_width // block,),
        in_specs=[fixed(tiles, local_rows, depth)] * groups
        + [
            fixed(groups, local_rows, HS),
            fixed(groups, local_rows, HS),
            pl.BlockSpec((depth, block), lambda i: (0, i)),
            pl.BlockSpec((1, block), lambda i: (0, i)),
            pl.BlockSpec((1, block), lambda i: (0, i)),
            pl.BlockSpec((block, outs), lambda i: (i, 0)),
        ],
        out_specs=out_specs,
        out_shape=out_shape,
        scratch_shapes=[
            pltpu.VMEM((groups * each, depth), jnp.bfloat16),
            pltpu.VMEM((groups * each, outs), jnp.float32),
            pltpu.VMEM((groups * each, 1), jnp.float32),
        ],
        compiler_params=pltpu.CompilerParams(dimension_semantics=("arbitrary",)),
        cost_estimate=pl.CostEstimate(
            flops=2 * groups * each * model_width * (depth + outs),
            bytes_accessed=2 * model_width * (depth + outs),
            transcendentals=0,
        ),
    )(*chunks, cosine, sine, w_proj, bias, gain, all_qkv)


def attend_kernel(counts_ref, image_ref, text_ref, out_ref, rows_ref, *, order):
    tile = pl.program_id(0)
    patch = counts_ref[0, tile]
    texts = counts_ref[1, tile]
    mine = counts_ref[2, 0]
    length = patch + texts
    parts, local_rows, outs = rows_ref.shape
    for at, s in enumerate(order):
        rows_ref[lax.rem(mine + (parts - s), parts)] = image_ref[at, 0]
    rows = parts * local_rows
    row = lax.broadcasted_iota(jnp.int32, (rows, WINDOW), 0)
    place = lax.broadcasted_iota(jnp.int32, (rows, WINDOW), 1)
    placing = jnp.where((row == patch + place) & (place < texts), 1.0, 0.0).astype(jnp.bfloat16)
    placed = jnp.dot(placing, text_ref[...], preferred_element_type=jnp.float32)
    image_row = lax.broadcasted_iota(jnp.int32, (rows, outs), 0) < patch
    qkv = jnp.where(
        image_row, rows_ref[...].reshape(rows, outs).astype(jnp.float32), placed
    ).astype(jnp.bfloat16)
    keys = qkv[:, GROUP * HS : (GROUP + 1) * HS]
    values = qkv[:, (GROUP + 1) * HS :]
    at_row = lax.broadcasted_iota(jnp.int32, (rows, rows), 0)
    at_col = lax.broadcasted_iota(jnp.int32, (rows, rows), 1)
    allowed = (at_col <= at_row) & (at_col < length)
    for g in range(GROUP):
        scores = lax.dot_general(
            qkv[:, g * HS : (g + 1) * HS],
            keys,
            (((1,), (1,)), ((), ())),
            preferred_element_type=jnp.float32,
        ) * (1.0 / math.sqrt(HS))
        scores = jnp.where(allowed, scores, -1e30)
        row_max = jnp.max(scores, axis=1, keepdims=True)
        weights = jnp.where(allowed, jnp.exp(scores - row_max), 0.0)
        probabilities = (weights / jnp.sum(weights, axis=1, keepdims=True)).astype(jnp.bfloat16)
        attended = jnp.dot(probabilities, values, preferred_element_type=jnp.float32)
        out_ref[:, :, :, g * HS : (g + 1) * HS] = attended.astype(jnp.bfloat16).reshape(
            parts, 1, local_rows, HS
        )


def attend(image_qkv, order, text_qkv, counts):
    parts, tiles, local_rows, outs = image_qkv.shape
    rows = parts * local_rows
    return pl.pallas_call(
        functools.partial(attend_kernel, order=order),
        grid_spec=pltpu.PrefetchScalarGridSpec(
            num_scalar_prefetch=1,
            grid=(tiles,),
            in_specs=[
                pl.BlockSpec((parts, 1, local_rows, outs), lambda t, c: (0, t, 0, 0)),
                pl.BlockSpec((WINDOW, outs), lambda t, c: (t, 0)),
            ],
            out_specs=pl.BlockSpec((parts, 1, local_rows, GROUP * HS), lambda t, c: (0, t, 0, 0)),
            scratch_shapes=[pltpu.VMEM((parts, local_rows, outs), jnp.bfloat16)],
        ),
        out_shape=jax.ShapeDtypeStruct((parts, tiles, local_rows, GROUP * HS), jnp.bfloat16),
        compiler_params=pltpu.CompilerParams(dimension_semantics=("arbitrary",)),
        cost_estimate=pl.CostEstimate(
            flops=tiles * rows * (2 * WINDOW * outs + 4 * GROUP * rows * HS),
            bytes_accessed=4 * tiles * rows * outs,
            transcendentals=tiles * GROUP * rows * rows,
        ),
    )(counts, image_qkv, text_qkv)


def out_kernel(att_ref, weight_hbm, hidden_ref, out_ref, rows_ref, weight_ref, sems):
    heads, _, head_width = att_ref.shape
    blocks, _, width = weight_ref.shape
    pieces = sems.shape[0]
    each = blocks // pieces
    copies = [
        pltpu.make_async_copy(
            weight_hbm.at[i * each : (i + 1) * each],
            weight_ref.at[i * each : (i + 1) * each],
            sems.at[i],
        )
        for i in range(pieces)
    ]
    for copy in copies:
        copy.start()
    for h in range(heads):
        rows_ref[:, h * head_width : (h + 1) * head_width] = att_ref[h]
    for i, copy in enumerate(copies):
        copy.wait()
        weights = jnp.concatenate([weight_ref[i * each + j] for j in range(each)], axis=1)
        total = jnp.dot(rows_ref[...], weights, preferred_element_type=jnp.float32)
        cols = slice(i * each * width, (i + 1) * each * width)
        out_ref[:, cols] = (hidden_ref[:, cols].astype(jnp.float32) + total).astype(jnp.bfloat16)


def project_out(attended, weight_blocks, hidden):
    _, rows, _ = attended.shape
    blocks, depth, width = weight_blocks.shape
    whole = pl.BlockSpec(memory_space=pltpu.VMEM)
    return pl.pallas_call(
        out_kernel,
        in_specs=[whole, pl.BlockSpec(memory_space=pl.ANY), whole],
        out_specs=whole,
        out_shape=jax.ShapeDtypeStruct((rows, blocks * width), jnp.bfloat16),
        scratch_shapes=[
            pltpu.VMEM((rows, depth), jnp.bfloat16),
            pltpu.VMEM((blocks, depth, width), jnp.bfloat16),
            pltpu.SemaphoreType.DMA((blocks // 4,)),
        ],
        cost_estimate=pl.CostEstimate(
            flops=2 * rows * depth * blocks * width,
            bytes_accessed=2 * depth * blocks * width,
            transcendentals=0,
        ),
    )(attended, weight_blocks, hidden)


def body(
    vit_features,
    patch_counts,
    text_counts,
    tile_dest,
    text_embeds,
    w_proj,
    b_proj,
    norm_gain,
    w_qkv,
    w_out,
):
    parts = lax.axis_size("mp")
    mine = lax.axis_index("mp")
    image_count, local_rows, _ = vit_features.shape
    model_width = text_embeds.shape[-1]
    slice_width = model_width // parts
    each = image_count * local_rows
    lengths = patch_counts + text_counts
    counts = jnp.stack([patch_counts, text_counts, jnp.full((image_count,), mine, jnp.int32)])

    all_qkv = lax.all_gather(w_qkv[0, :, 0], "dp", axis=0, tiled=True)

    payload = pack(text_embeds, w_out[0, 0], mine, parts)
    got = [payload[0]] + [shifted(payload[s], "mp", s) for s in range(1, parts)]
    window, all_heads = unpack(got, counts, image_count, slice_width, w_out.shape[3])
    all_out = lax.all_gather(all_heads[None], "dp", axis=0, tiled=True)

    arrived = exchange_tiles(vit_features, tile_dest)
    chunks = ring_chunks(arrived, "mp", -(-IMAGE_ROWS // local_rows))
    text_chunks = ring_chunks(window, "mp")

    text_places = patch_counts[:, None] + jnp.arange(WINDOW, dtype=jnp.int32)[None, :]
    text_cos, text_sin = rotation_tables(text_places.reshape(-1))
    order = (0, *[s for k in range(1, parts // 2) for s in (k, parts - k)], parts // 2)
    local = jnp.arange(local_rows, dtype=jnp.int32)
    begins = jnp.stack([lax.rem(mine + (parts - s), parts) * local_rows for s in order])
    chunk_cos, chunk_sin = rotation_tables(begins[:, None] + local[None, :])

    bias = b_proj.reshape(1, model_width)
    image_qkv, own_projected = image_qkv_of(
        [chunks[s] for s in order], chunk_cos, chunk_sin, w_proj, bias, norm_gain, all_qkv
    )
    text_qkv = text_qkv_of(text_chunks, mine, text_cos, text_sin, norm_gain, all_qkv)

    own_rows = (mine * local_rows + local)[None, :, None]
    hidden = jnp.where(
        own_rows < patch_counts[:, None, None],
        own_projected.reshape(image_count, local_rows, model_width),
        jnp.where(
            own_rows < lengths[:, None, None], text_embeds, jnp.zeros_like(text_embeds)
        ),
    ).reshape(each, model_width)

    attended = attend(image_qkv, order, text_qkv, counts)
    returned = lax.all_to_all(
        attended.reshape(parts, each, -1), "mp", split_axis=0, concat_axis=0, tiled=True
    )
    out = project_out(returned, all_out, hidden)
    return out.reshape(image_count, local_rows, model_width)


def solution(mesh):
    in_specs = (
        P("dp", "mp", None),
        P("dp"),
        P("dp"),
        P("dp"),
        P("dp", "mp", None),
        P(),
        P(),
        P(),
        P(None, "dp", "mp", None),
        P(None, "mp", None, "dp"),
    )
    out_specs = P("dp", "mp", None)

    return jax.shard_map(body, mesh=mesh, in_specs=in_specs, out_specs=out_specs, check_vma=False)
```

```python
import functools
import math

import jax
import jax.numpy as jnp
from jax import lax
from jax.experimental import pallas as pl
from jax.experimental.pallas import tpu as pltpu
from jax.sharding import PartitionSpec as P


HS = 128
GROUP = 2
WINDOW = 64
IMAGE_ROWS = 192
EXTRA = 128

rope_base = 500000.0
epsilon = 1e-05


def shifted(value, axis, step, sources=None):
    size = lax.axis_size(axis)
    pairs = [(i, (i + step) % size) for i in range(size) if sources is None or i in sources]
    return lax.ppermute(value, axis, pairs)


def ring_chunks(own, axis, useful=None):
    size = lax.axis_size(axis)
    useful = size if useful is None else useful
    chunks = [own] + [None] * (size - 1)
    for s in range(1, size // 2 + 1):
        holders = [(o + s - 1) % size for o in range(useful)]
        chunks[s] = shifted(chunks[s - 1], axis, 1, holders)
        if s < size - s:
            holders = [(o - s + 1) % size for o in range(useful)]
            chunks[size - s] = shifted(chunks[(size - s + 1) % size], axis, -1, holders)
    return chunks


def rotation_tables(rows):
    half_size = HS // 2
    inverse = jnp.exp(
        -(2.0 * jnp.arange(half_size, dtype=jnp.float32) / HS) * math.log(rope_base)
    )
    angles = rows.astype(jnp.float32)[..., None] * inverse
    cosine, sine = jnp.cos(angles), jnp.sin(angles)
    return (
        jnp.concatenate([cosine, cosine], axis=-1),
        jnp.concatenate([-sine, sine], axis=-1),
    )


def rotate_store(joined, cosine, sine, store):
    heads = joined.shape[1] // HS
    for p in range(heads):
        part = joined[:, p * HS : (p + 1) * HS]
        if p < heads - 1:
            part = part * cosine + pltpu.roll(part, HS // 2, 1) * sine
        store(p, part.astype(jnp.bfloat16))


def order_kernel(got_ref, out_ref, *, image_count):
    total, wide = got_ref.shape
    width = wide - EXTRA
    dest = got_ref[:, width:].astype(jnp.float32)
    row = lax.broadcasted_iota(jnp.int32, (total, total), 0)
    col = lax.broadcasted_iota(jnp.int32, (total, total), 1)
    earlier = (dest == dest.T) & (col < row)
    slots = jnp.sum(jnp.where(earlier, 1.0, 0.0), axis=1, keepdims=True)
    targets = (dest * image_count + slots).T
    placing = jnp.where(targets == row.astype(jnp.float32), 1.0, 0.0).astype(jnp.bfloat16)
    out_ref[...] = jnp.dot(
        placing, got_ref[:, :width], preferred_element_type=jnp.float32
    ).astype(jnp.bfloat16)


def exchange_tiles(vit_features, tile_dest):
    image_count, _, width = vit_features.shape
    ranks = lax.axis_size("dp")
    by_row = jnp.moveaxis(vit_features, 1, 0)
    tags = jnp.broadcast_to(
        tile_dest.astype(jnp.bfloat16)[None, :, None], (ranks, image_count, EXTRA)
    )
    sent = jnp.concatenate([by_row, tags], axis=2)
    got = lax.all_to_all(sent, "dp", split_axis=0, concat_axis=0, tiled=True)
    total = ranks * image_count
    ordered = pl.pallas_call(
        functools.partial(order_kernel, image_count=image_count),
        out_shape=jax.ShapeDtypeStruct((total, width), jnp.bfloat16),
        cost_estimate=pl.CostEstimate(
            flops=2 * total * total * width, bytes_accessed=4 * total * width, transcendentals=0
        ),
    )(got.reshape(total, width + EXTRA))
    arrived = lax.all_to_all(
        ordered.reshape(ranks, image_count, width),
        "dp",
        split_axis=0,
        concat_axis=0,
        tiled=True,
    )
    return jnp.moveaxis(arrived, 0, 1)


def pack_kernel(place_ref, text_ref, heads_ref, *out_refs):
    parts = len(out_refs)
    rows, wide = out_refs[0].shape
    folds = heads_ref.shape[0] // rows
    cols = heads_ref.shape[1]
    width = wide - folds * cols
    mine = place_ref[0]
    for s, out_ref in enumerate(out_refs):
        at = pl.multiple_of(lax.rem(mine + s, parts) * width, width)
        out_ref[:, :width] = text_ref[:, :, pl.ds(at, width)].reshape(rows, width)
        for f in range(folds):
            out_ref[:, width + f * cols : width + (f + 1) * cols] = heads_ref[
                f * rows : (f + 1) * rows, :
            ]


def pack(text_embeds, head_rows, mine, parts):
    tiles, local_rows, model_width = text_embeds.shape
    rows = tiles * local_rows
    width = model_width // parts
    wide = width + head_rows.shape[0] * head_rows.shape[1] // rows
    whole = pl.BlockSpec(memory_space=pltpu.VMEM)
    return pl.pallas_call(
        pack_kernel,
        in_specs=[pl.BlockSpec(memory_space=pltpu.SMEM), whole, whole],
        out_specs=[whole] * parts,
        out_shape=[jax.ShapeDtypeStruct((rows, wide), jnp.bfloat16)] * parts,
        cost_estimate=pl.CostEstimate(
            flops=1 << 20, bytes_accessed=4 * parts * rows * wide, transcendentals=0
        ),
    )(mine.reshape(1), text_embeds, head_rows)


def unpack_kernel(counts_ref, *refs, tiles, width):
    parts = len(refs) - 3
    got_refs = refs[:parts]
    window_ref, heads_ref, rows_ref = refs[parts:]
    mine = counts_ref[2, 0]
    each, wide = got_refs[0].shape
    local_rows = each // tiles
    cols = heads_ref.shape[1]
    folds = (wide - width) // cols
    for s, got_ref in enumerate(got_refs):
        at = lax.rem(mine + (parts - s), parts)
        for f in range(folds):
            begin = pl.multiple_of((at * folds + f) * each, each)
            heads_ref[pl.ds(begin, each), :] = got_ref[:, width + f * cols : width + (f + 1) * cols]
        for t in range(tiles):
            rows_ref[t, at] = got_ref[t * local_rows : (t + 1) * local_rows, :width]
    rows = parts * local_rows
    place = lax.broadcasted_iota(jnp.int32, (WINDOW, rows), 0)
    row = lax.broadcasted_iota(jnp.int32, (WINDOW, rows), 1)
    for t in range(tiles):
        picks = (row == counts_ref[0, t] + place) & (place < counts_ref[1, t])
        window_ref[t * WINDOW : (t + 1) * WINDOW, :] = jnp.dot(
            jnp.where(picks, 1.0, 0.0).astype(jnp.bfloat16),
            rows_ref[t].reshape(rows, width),
            preferred_element_type=jnp.float32,
        ).astype(jnp.bfloat16)


def unpack(got, counts, tiles, width, cols):
    parts = len(got)
    each, wide = got[0].shape
    local_rows = each // tiles
    whole = pl.BlockSpec(memory_space=pltpu.VMEM)
    return pl.pallas_call(
        functools.partial(unpack_kernel, tiles=tiles, width=width),
        in_specs=[pl.BlockSpec(memory_space=pltpu.SMEM)] + [whole] * parts,
        out_specs=[whole, whole],
        out_shape=[
            jax.ShapeDtypeStruct((tiles * WINDOW, width), jnp.bfloat16),
            jax.ShapeDtypeStruct((parts * each * ((wide - width) // cols), cols), jnp.bfloat16),
        ],
        scratch_shapes=[pltpu.VMEM((tiles, parts, local_rows, width), jnp.bfloat16)],
        cost_estimate=pl.CostEstimate(
            flops=2 * tiles * WINDOW * parts * local_rows * width,
            bytes_accessed=2 * parts * each * wide,
            transcendentals=0,
        ),
    )(counts, *got)


def text_kernel(place_ref, *refs):
    parts = len(refs) - 5
    chunk_refs = refs[:parts]
    cos_ref, sin_ref, gain_ref, weight_ref, out_ref = refs[parts:]
    width = chunk_refs[0].shape[1]
    mine = place_ref[0]
    squares = None
    total = None
    for s, chunk_ref in enumerate(chunk_refs):
        at = lax.rem(mine + (parts - s), parts)
        rows = chunk_ref[...].astype(jnp.float32)
        part = jnp.sum(rows * rows, axis=1, keepdims=True)
        squares = part if squares is None else squares + part
        scaled = (rows * gain_ref[pl.ds(at, 1), :]).astype(jnp.bfloat16)
        block = weight_ref[pl.ds(pl.multiple_of(at * width, width), width), :]
        term = jnp.dot(scaled, block, preferred_element_type=jnp.float32)
        total = term if total is None else total + term
    scale = lax.rsqrt(squares * (1.0 / (parts * width)) + epsilon)

    def store(p, value):
        out_ref[:, p * HS : (p + 1) * HS] = value

    rotate_store(total * scale, cos_ref[...], sin_ref[...], store)


def text_qkv_of(chunks, mine, cosine, sine, gain, all_qkv):
    rows, width = chunks[0].shape
    parts = len(chunks)
    outs = all_qkv.shape[1]
    whole = pl.BlockSpec(memory_space=pltpu.VMEM)
    return pl.pallas_call(
        text_kernel,
        in_specs=[pl.BlockSpec(memory_space=pltpu.SMEM)] + [whole] * (parts + 4),
        out_specs=whole,
        out_shape=jax.ShapeDtypeStruct((rows, outs), jnp.bfloat16),
        cost_estimate=pl.CostEstimate(
            flops=2 * rows * parts * width * outs,
            bytes_accessed=2 * parts * width * (rows + outs),
            transcendentals=0,
        ),
    )(mine.reshape(1), *chunks, cosine, sine, gain.reshape(parts, width), all_qkv)


def image_kernel(place_ref, *refs, groups, useful):
    chunk_refs = refs[:groups]
    cos_ref, sin_ref, proj_ref, bias_ref, gain_ref, qkv_ref = refs[groups : groups + 6]
    out_ref, hidden_ref, rows_ref, sum_ref, squares_ref = refs[groups + 6 :]
    tiles, local_rows, depth = chunk_refs[0].shape
    each = tiles * local_rows
    step = pl.program_id(0)
    mine = place_ref[0]

    @pl.when(step == 0)
    def _():
        for s, chunk_ref in enumerate(chunk_refs):
            at = lax.rem(mine + (groups - s), groups)

            @pl.when(at < useful)
            def _(at=at, chunk_ref=chunk_ref):
                begin = pl.multiple_of(at * each, each)
                rows_ref[pl.ds(begin, each), :] = chunk_ref[...].reshape(each, depth)

        sum_ref[...] = jnp.zeros_like(sum_ref)
        squares_ref[...] = jnp.zeros_like(squares_ref)

    projected = (
        jnp.dot(rows_ref[...], proj_ref[...], preferred_element_type=jnp.float32) + bias_ref[...]
    ).astype(jnp.bfloat16)
    for at in range(useful):

        @pl.when(mine == at)
        def _(at=at):
            hidden_ref[...] = projected[at * each : (at + 1) * each]

    @pl.when(mine >= useful)
    def _():
        hidden_ref[...] = jnp.zeros_like(hidden_ref)

    wide = projected.astype(jnp.float32)
    squares_ref[...] += jnp.sum(wide * wide, axis=1, keepdims=True)
    scaled = (wide * gain_ref[...]).astype(jnp.bfloat16)
    sum_ref[...] += jnp.dot(scaled, qkv_ref[...], preferred_element_type=jnp.float32)

    @pl.when(step == pl.num_programs(0) - 1)
    def _():
        model_width = proj_ref.shape[1] * pl.num_programs(0)
        scale = lax.rsqrt(squares_ref[...] * (1.0 / model_width) + epsilon)
        shape = (useful, tiles, local_rows, HS)
        cosine = jnp.broadcast_to(cos_ref[...][:, None], shape).reshape(useful * each, HS)
        sine = jnp.broadcast_to(sin_ref[...][:, None], shape).reshape(useful * each, HS)

        def store(p, value):
            out_ref[:, :, :, p * HS : (p + 1) * HS] = value.reshape(shape)

        rotate_store(sum_ref[...] * scale, cosine, sine, store)


def image_qkv_of(chunks, mine, cosine, sine, w_proj, bias, gain, all_qkv):
    groups = len(chunks)
    useful = cosine.shape[0]
    tiles, local_rows, depth = chunks[0].shape
    model_width, outs = all_qkv.shape
    each = tiles * local_rows
    block = 1024
    fixed = lambda *shape: pl.BlockSpec(shape, lambda i, c: (0,) * len(shape))
    return pl.pallas_call(
        functools.partial(image_kernel, groups=groups, useful=useful),
        grid_spec=pltpu.PrefetchScalarGridSpec(
            num_scalar_prefetch=1,
            grid=(model_width // block,),
            in_specs=[fixed(tiles, local_rows, depth)] * groups
            + [
                fixed(useful, local_rows, HS),
                fixed(useful, local_rows, HS),
                pl.BlockSpec((depth, block), lambda i, c: (0, i)),
                pl.BlockSpec((1, block), lambda i, c: (0, i)),
                pl.BlockSpec((1, block), lambda i, c: (0, i)),
                pl.BlockSpec((block, outs), lambda i, c: (i, 0)),
            ],
            out_specs=[
                fixed(useful, tiles, local_rows, outs),
                pl.BlockSpec((each, block), lambda i, c: (0, i)),
            ],
            scratch_shapes=[
                pltpu.VMEM((useful * each, depth), jnp.bfloat16),
                pltpu.VMEM((useful * each, outs), jnp.float32),
                pltpu.VMEM((useful * each, 1), jnp.float32),
            ],
        ),
        out_shape=[
            jax.ShapeDtypeStruct((useful, tiles, local_rows, outs), jnp.bfloat16),
            jax.ShapeDtypeStruct((each, model_width), jnp.bfloat16),
        ],
        compiler_params=pltpu.CompilerParams(dimension_semantics=("arbitrary",)),
        cost_estimate=pl.CostEstimate(
            flops=2 * useful * each * model_width * (depth + outs),
            bytes_accessed=2 * model_width * (depth + outs),
            transcendentals=0,
        ),
    )(mine.reshape(1), *chunks, cosine, sine, w_proj, bias, gain, all_qkv)


def attend_kernel(counts_ref, image_ref, text_ref, out_ref):
    tile = pl.program_id(0)
    patch = counts_ref[0, tile]
    texts = counts_ref[1, tile]
    length = patch + texts
    useful, _, local_rows, outs = image_ref.shape
    parts = out_ref.shape[0]
    rows = parts * local_rows
    row = lax.broadcasted_iota(jnp.int32, (rows, WINDOW), 0)
    place = lax.broadcasted_iota(jnp.int32, (rows, WINDOW), 1)
    placing = jnp.where((row == patch + place) & (place < texts), 1.0, 0.0).astype(jnp.bfloat16)
    placed = jnp.dot(placing, text_ref[...], preferred_element_type=jnp.float32)
    first = useful * local_rows
    image_row = lax.broadcasted_iota(jnp.int32, (first, outs), 0) < patch
    image = image_ref[...].reshape(first, outs).astype(jnp.float32)
    qkv = jnp.concatenate(
        [jnp.where(image_row, image, placed[:first]), placed[first:]], axis=0
    ).astype(jnp.bfloat16)
    keys = qkv[:, GROUP * HS : (GROUP + 1) * HS]
    values = qkv[:, (GROUP + 1) * HS :]
    at_row = lax.broadcasted_iota(jnp.int32, (rows, rows), 0)
    at_col = lax.broadcasted_iota(jnp.int32, (rows, rows), 1)
    allowed = (at_col <= at_row) & (at_col < length)
    for g in range(GROUP):
        scores = lax.dot_general(
            qkv[:, g * HS : (g + 1) * HS],
            keys,
            (((1,), (1,)), ((), ())),
            preferred_element_type=jnp.float32,
        ) * (1.0 / math.sqrt(HS))
        scores = jnp.where(allowed, scores, -1e30)
        row_max = jnp.max(scores, axis=1, keepdims=True)
        weights = jnp.where(allowed, jnp.exp(scores - row_max), 0.0)
        probabilities = (weights / jnp.sum(weights, axis=1, keepdims=True)).astype(jnp.bfloat16)
        attended = jnp.dot(probabilities, values, preferred_element_type=jnp.float32)
        out_ref[:, :, :, g * HS : (g + 1) * HS] = attended.astype(jnp.bfloat16).reshape(
            parts, 1, local_rows, HS
        )


def attend(image_qkv, text_qkv, counts, parts):
    useful, tiles, local_rows, outs = image_qkv.shape
    rows = parts * local_rows
    return pl.pallas_call(
        attend_kernel,
        grid_spec=pltpu.PrefetchScalarGridSpec(
            num_scalar_prefetch=1,
            grid=(tiles,),
            in_specs=[
                pl.BlockSpec((useful, 1, local_rows, outs), lambda t, c: (0, t, 0, 0)),
                pl.BlockSpec((WINDOW, outs), lambda t, c: (t, 0)),
            ],
            out_specs=pl.BlockSpec((parts, 1, local_rows, GROUP * HS), lambda t, c: (0, t, 0, 0)),
        ),
        out_shape=jax.ShapeDtypeStruct((parts, tiles, local_rows, GROUP * HS), jnp.bfloat16),
        compiler_params=pltpu.CompilerParams(dimension_semantics=("arbitrary",)),
        cost_estimate=pl.CostEstimate(
            flops=tiles * rows * (2 * WINDOW * outs + 4 * GROUP * rows * HS),
            bytes_accessed=4 * tiles * rows * outs,
            transcendentals=tiles * GROUP * rows * rows,
        ),
    )(counts, image_qkv, text_qkv)


def out_kernel(att_ref, weight_hbm, hidden_ref, out_ref, rows_ref, weight_ref, sems):
    heads, _, head_width = att_ref.shape
    blocks, _, width = weight_ref.shape
    pieces = sems.shape[0]
    each = blocks // pieces
    copies = [
        pltpu.make_async_copy(
            weight_hbm.at[i * each : (i + 1) * each],
            weight_ref.at[i * each : (i + 1) * each],
            sems.at[i],
        )
        for i in range(pieces)
    ]
    for copy in copies:
        copy.start()
    for h in range(heads):
        rows_ref[:, h * head_width : (h + 1) * head_width] = att_ref[h]
    for i, copy in enumerate(copies):
        copy.wait()
        weights = jnp.concatenate([weight_ref[i * each + j] for j in range(each)], axis=1)
        total = jnp.dot(rows_ref[...], weights, preferred_element_type=jnp.float32)
        cols = slice(i * each * width, (i + 1) * each * width)
        out_ref[:, cols] = (hidden_ref[:, cols].astype(jnp.float32) + total).astype(jnp.bfloat16)


def project_out(attended, weight_blocks, hidden):
    _, rows, _ = attended.shape
    blocks, depth, width = weight_blocks.shape
    whole = pl.BlockSpec(memory_space=pltpu.VMEM)
    return pl.pallas_call(
        out_kernel,
        in_specs=[whole, pl.BlockSpec(memory_space=pl.ANY), whole],
        out_specs=whole,
        out_shape=jax.ShapeDtypeStruct((rows, blocks * width), jnp.bfloat16),
        scratch_shapes=[
            pltpu.VMEM((rows, depth), jnp.bfloat16),
            pltpu.VMEM((blocks, depth, width), jnp.bfloat16),
            pltpu.SemaphoreType.DMA((blocks // 4,)),
        ],
        cost_estimate=pl.CostEstimate(
            flops=2 * rows * depth * blocks * width,
            bytes_accessed=2 * depth * blocks * width,
            transcendentals=0,
        ),
    )(attended, weight_blocks, hidden)


def body(
    vit_features,
    patch_counts,
    text_counts,
    tile_dest,
    text_embeds,
    w_proj,
    b_proj,
    norm_gain,
    w_qkv,
    w_out,
):
    parts = lax.axis_size("mp")
    mine = lax.axis_index("mp")
    image_count, local_rows, _ = vit_features.shape
    model_width = text_embeds.shape[-1]
    slice_width = model_width // parts
    each = image_count * local_rows
    lengths = patch_counts + text_counts
    counts = jnp.stack([patch_counts, text_counts, jnp.full((image_count,), mine, jnp.int32)])

    all_qkv = lax.all_gather(w_qkv[0, :, 0], "dp", axis=0, tiled=True)

    payload = pack(text_embeds, w_out[0, 0], mine, parts)
    got = [payload[0]] + [shifted(payload[s], "mp", s) for s in range(1, parts)]
    window, all_heads = unpack(got, counts, image_count, slice_width, w_out.shape[3])
    all_out = lax.all_gather(all_heads[None], "dp", axis=0, tiled=True)

    arrived = exchange_tiles(vit_features, tile_dest)
    chunks = ring_chunks(arrived, "mp", -(-IMAGE_ROWS // local_rows))
    text_chunks = ring_chunks(window, "mp")

    text_places = patch_counts[:, None] + jnp.arange(WINDOW, dtype=jnp.int32)[None, :]
    text_cos, text_sin = rotation_tables(text_places.reshape(-1))
    local = jnp.arange(local_rows, dtype=jnp.int32)
    useful = -(-IMAGE_ROWS // local_rows)
    chunk_cos, chunk_sin = rotation_tables(
        jnp.arange(useful * local_rows, dtype=jnp.int32).reshape(useful, local_rows)
    )

    bias = b_proj.reshape(1, model_width)
    image_qkv, own_projected = image_qkv_of(
        chunks, mine, chunk_cos, chunk_sin, w_proj, bias, norm_gain, all_qkv
    )
    text_qkv = text_qkv_of(text_chunks, mine, text_cos, text_sin, norm_gain, all_qkv)

    own_rows = (mine * local_rows + local)[None, :, None]
    hidden = jnp.where(
        own_rows < patch_counts[:, None, None],
        own_projected.reshape(image_count, local_rows, model_width),
        jnp.where(
            own_rows < lengths[:, None, None], text_embeds, jnp.zeros_like(text_embeds)
        ),
    ).reshape(each, model_width)

    attended = attend(image_qkv, text_qkv, counts, parts)
    returned = lax.all_to_all(
        attended.reshape(parts, each, -1), "mp", split_axis=0, concat_axis=0, tiled=True
    )
    out = project_out(returned, all_out, hidden)
    return out.reshape(image_count, local_rows, model_width)


def solution(mesh):
    in_specs = (
        P("dp", "mp", None),
        P("dp"),
        P("dp"),
        P("dp"),
        P("dp", "mp", None),
        P(),
        P(),
        P(),
        P(None, "dp", "mp", None),
        P(None, "mp", None, "dp"),
    )
    out_specs = P("dp", "mp", None)

    return jax.shard_map(body, mesh=mesh, in_specs=in_specs, out_specs=out_specs, check_vma=False)
```

```python
import functools
import math

import jax
import jax.numpy as jnp
from jax import lax
from jax.experimental import pallas as pl
from jax.experimental.pallas import tpu as pltpu
from jax.sharding import PartitionSpec as P


HS = 128
GROUP = 2
WINDOW = 64
IMAGE_ROWS = 192
EXTRA = 128

rope_base = 500000.0
epsilon = 1e-05


def shifted(value, axis, step, sources=None):
    size = lax.axis_size(axis)
    pairs = [(i, (i + step) % size) for i in range(size) if sources is None or i in sources]
    return lax.ppermute(value, axis, pairs)


def ring_chunks(own, axis, useful=None):
    size = lax.axis_size(axis)
    useful = size if useful is None else useful
    chunks = [own] + [None] * (size - 1)
    for s in range(1, size // 2 + 1):
        holders = [(o + s - 1) % size for o in range(useful)]
        chunks[s] = shifted(chunks[s - 1], axis, 1, holders)
        if s < size - s:
            holders = [(o - s + 1) % size for o in range(useful)]
            chunks[size - s] = shifted(chunks[(size - s + 1) % size], axis, -1, holders)
    return chunks


def rotation_tables(rows):
    half_size = HS // 2
    inverse = jnp.exp(
        -(2.0 * jnp.arange(half_size, dtype=jnp.float32) / HS) * math.log(rope_base)
    )
    angles = rows.astype(jnp.float32)[..., None] * inverse
    cosine, sine = jnp.cos(angles), jnp.sin(angles)
    return (
        jnp.concatenate([cosine, cosine], axis=-1),
        jnp.concatenate([-sine, sine], axis=-1),
    )


def rotate_store(joined, cosine, sine, store):
    heads = joined.shape[1] // HS
    for p in range(heads):
        part = joined[:, p * HS : (p + 1) * HS]
        if p < heads - 1:
            part = part * cosine + pltpu.roll(part, HS // 2, 1) * sine
        store(p, part.astype(jnp.bfloat16))


def order_kernel(got_ref, out_ref, *, image_count):
    total, wide = got_ref.shape
    width = wide - EXTRA
    dest = got_ref[:, width:].astype(jnp.float32)
    row = lax.broadcasted_iota(jnp.int32, (total, total), 0)
    col = lax.broadcasted_iota(jnp.int32, (total, total), 1)
    earlier = (dest == dest.T) & (col < row)
    slots = jnp.sum(jnp.where(earlier, 1.0, 0.0), axis=1, keepdims=True)
    targets = (dest * image_count + slots).T
    placing = jnp.where(targets == row.astype(jnp.float32), 1.0, 0.0).astype(jnp.bfloat16)
    out_ref[...] = jnp.dot(
        placing, got_ref[:, :width], preferred_element_type=jnp.float32
    ).astype(jnp.bfloat16)


def exchange_tiles(vit_features, tile_dest):
    image_count, _, width = vit_features.shape
    ranks = lax.axis_size("dp")
    by_row = jnp.moveaxis(vit_features, 1, 0)
    tags = jnp.broadcast_to(
        tile_dest.astype(jnp.bfloat16)[None, :, None], (ranks, image_count, EXTRA)
    )
    sent = jnp.concatenate([by_row, tags], axis=2)
    got = lax.all_to_all(sent, "dp", split_axis=0, concat_axis=0, tiled=True)
    total = ranks * image_count
    ordered = pl.pallas_call(
        functools.partial(order_kernel, image_count=image_count),
        out_shape=jax.ShapeDtypeStruct((total, width), jnp.bfloat16),
        cost_estimate=pl.CostEstimate(
            flops=2 * total * total * width, bytes_accessed=4 * total * width, transcendentals=0
        ),
    )(got.reshape(total, width + EXTRA))
    arrived = lax.all_to_all(
        ordered.reshape(ranks, image_count, width),
        "dp",
        split_axis=0,
        concat_axis=0,
        tiled=True,
    )
    return jnp.moveaxis(arrived, 0, 1)


def pack_kernel(place_ref, text_ref, heads_ref, *out_refs):
    parts = len(out_refs)
    rows, wide = out_refs[0].shape
    folds = heads_ref.shape[0] // rows
    cols = heads_ref.shape[1]
    width = wide - folds * cols
    mine = place_ref[0]
    for s, out_ref in enumerate(out_refs):
        at = pl.multiple_of(lax.rem(mine + s, parts) * width, width)
        out_ref[:, :width] = text_ref[:, :, pl.ds(at, width)].reshape(rows, width)
        for f in range(folds):
            out_ref[:, width + f * cols : width + (f + 1) * cols] = heads_ref[
                f * rows : (f + 1) * rows, :
            ]


def pack(text_embeds, head_rows, mine, parts):
    tiles, local_rows, model_width = text_embeds.shape
    rows = tiles * local_rows
    width = model_width // parts
    wide = width + head_rows.shape[0] * head_rows.shape[1] // rows
    whole = pl.BlockSpec(memory_space=pltpu.VMEM)
    return pl.pallas_call(
        pack_kernel,
        in_specs=[pl.BlockSpec(memory_space=pltpu.SMEM), whole, whole],
        out_specs=[whole] * parts,
        out_shape=[jax.ShapeDtypeStruct((rows, wide), jnp.bfloat16)] * parts,
        cost_estimate=pl.CostEstimate(
            flops=1 << 20, bytes_accessed=4 * parts * rows * wide, transcendentals=0
        ),
    )(mine.reshape(1), text_embeds, head_rows)


def unpack_kernel(counts_ref, *refs, tiles, width):
    parts = len(refs) - 3
    got_refs = refs[:parts]
    window_ref, heads_ref, rows_ref = refs[parts:]
    mine = counts_ref[2, 0]
    each, wide = got_refs[0].shape
    local_rows = each // tiles
    cols = heads_ref.shape[1]
    folds = (wide - width) // cols
    for s, got_ref in enumerate(got_refs):
        at = lax.rem(mine + (parts - s), parts)
        for f in range(folds):
            begin = pl.multiple_of((at * folds + f) * each, each)
            heads_ref[pl.ds(begin, each), :] = got_ref[:, width + f * cols : width + (f + 1) * cols]
        for t in range(tiles):
            rows_ref[t, at] = got_ref[t * local_rows : (t + 1) * local_rows, :width]
    rows = parts * local_rows
    place = lax.broadcasted_iota(jnp.int32, (WINDOW, rows), 0)
    row = lax.broadcasted_iota(jnp.int32, (WINDOW, rows), 1)
    for t in range(tiles):
        picks = (row == counts_ref[0, t] + place) & (place < counts_ref[1, t])
        window_ref[t * WINDOW : (t + 1) * WINDOW, :] = jnp.dot(
            jnp.where(picks, 1.0, 0.0).astype(jnp.bfloat16),
            rows_ref[t].reshape(rows, width),
            preferred_element_type=jnp.float32,
        ).astype(jnp.bfloat16)


def unpack(got, counts, tiles, width, cols):
    parts = len(got)
    each, wide = got[0].shape
    local_rows = each // tiles
    whole = pl.BlockSpec(memory_space=pltpu.VMEM)
    return pl.pallas_call(
        functools.partial(unpack_kernel, tiles=tiles, width=width),
        in_specs=[pl.BlockSpec(memory_space=pltpu.SMEM)] + [whole] * parts,
        out_specs=[whole, whole],
        out_shape=[
            jax.ShapeDtypeStruct((tiles * WINDOW, width), jnp.bfloat16),
            jax.ShapeDtypeStruct((parts * each * ((wide - width) // cols), cols), jnp.bfloat16),
        ],
        scratch_shapes=[pltpu.VMEM((tiles, parts, local_rows, width), jnp.bfloat16)],
        cost_estimate=pl.CostEstimate(
            flops=2 * tiles * WINDOW * parts * local_rows * width,
            bytes_accessed=2 * parts * each * wide,
            transcendentals=0,
        ),
    )(counts, *got)


def text_kernel(place_ref, *refs):
    parts = len(refs) - 7
    chunk_refs = refs[:parts]
    cos_ref, sin_ref, gain_ref, weight_hbm, out_ref, weight_ref, sems = refs[parts:]
    width = chunk_refs[0].shape[1]
    mine = place_ref[0]
    copies = []
    for s in range(parts):
        begin = pl.multiple_of(lax.rem(mine + (parts - s), parts) * width, width)
        copies.append(
            pltpu.make_async_copy(
                weight_hbm.at[pl.ds(begin, width)], weight_ref.at[s], sems.at[s]
            )
        )
    for copy in copies:
        copy.start()
    squares = None
    total = None
    for s, chunk_ref in enumerate(chunk_refs):
        at = lax.rem(mine + (parts - s), parts)
        rows = chunk_ref[...].astype(jnp.float32)
        part = jnp.sum(rows * rows, axis=1, keepdims=True)
        squares = part if squares is None else squares + part
        scaled = (rows * gain_ref[pl.ds(at, 1), :]).astype(jnp.bfloat16)
        copies[s].wait()
        term = jnp.dot(scaled, weight_ref[s], preferred_element_type=jnp.float32)
        total = term if total is None else total + term
    scale = lax.rsqrt(squares * (1.0 / (parts * width)) + epsilon)

    def store(p, value):
        out_ref[:, p * HS : (p + 1) * HS] = value

    rotate_store(total * scale, cos_ref[...], sin_ref[...], store)


def text_qkv_of(chunks, mine, cosine, sine, gain, all_qkv):
    rows, width = chunks[0].shape
    parts = len(chunks)
    outs = all_qkv.shape[1]
    whole = pl.BlockSpec(memory_space=pltpu.VMEM)
    return pl.pallas_call(
        text_kernel,
        in_specs=[pl.BlockSpec(memory_space=pltpu.SMEM)]
        + [whole] * (parts + 3)
        + [pl.BlockSpec(memory_space=pl.ANY)],
        out_specs=whole,
        out_shape=jax.ShapeDtypeStruct((rows, outs), jnp.bfloat16),
        scratch_shapes=[
            pltpu.VMEM((parts, width, outs), jnp.bfloat16),
            pltpu.SemaphoreType.DMA((parts,)),
        ],
        cost_estimate=pl.CostEstimate(
            flops=2 * rows * parts * width * outs,
            bytes_accessed=2 * parts * width * (rows + outs),
            transcendentals=0,
        ),
    )(mine.reshape(1), *chunks, cosine, sine, gain.reshape(parts, width), all_qkv)


def image_kernel(place_ref, *refs, groups, useful):
    chunk_refs = refs[:groups]
    cos_ref, sin_ref, proj_ref, bias_ref, gain_ref, qkv_ref = refs[groups : groups + 6]
    out_ref, hidden_ref, rows_ref, sum_ref, squares_ref = refs[groups + 6 :]
    tiles, local_rows, depth = chunk_refs[0].shape
    each = tiles * local_rows
    step = pl.program_id(0)
    mine = place_ref[0]

    @pl.when(step == 0)
    def _():
        for s, chunk_ref in enumerate(chunk_refs):
            at = lax.rem(mine + (groups - s), groups)

            @pl.when(at < useful)
            def _(at=at, chunk_ref=chunk_ref):
                begin = pl.multiple_of(at * each, each)
                rows_ref[pl.ds(begin, each), :] = chunk_ref[...].reshape(each, depth)

        sum_ref[...] = jnp.zeros_like(sum_ref)
        squares_ref[...] = jnp.zeros_like(squares_ref)

    projected = (
        jnp.dot(rows_ref[...], proj_ref[...], preferred_element_type=jnp.float32) + bias_ref[...]
    ).astype(jnp.bfloat16)
    for at in range(useful):

        @pl.when(mine == at)
        def _(at=at):
            hidden_ref[...] = projected[at * each : (at + 1) * each]

    @pl.when(mine >= useful)
    def _():
        hidden_ref[...] = jnp.zeros_like(hidden_ref)

    wide = projected.astype(jnp.float32)
    squares_ref[...] += jnp.sum(wide * wide, axis=1, keepdims=True)
    scaled = (wide * gain_ref[...]).astype(jnp.bfloat16)
    sum_ref[...] += jnp.dot(scaled, qkv_ref[...], preferred_element_type=jnp.float32)

    @pl.when(step == pl.num_programs(0) - 1)
    def _():
        model_width = proj_ref.shape[1] * pl.num_programs(0)
        scale = lax.rsqrt(squares_ref[...] * (1.0 / model_width) + epsilon)
        shape = (useful, tiles, local_rows, HS)
        cosine = jnp.broadcast_to(cos_ref[...][:, None], shape).reshape(useful * each, HS)
        sine = jnp.broadcast_to(sin_ref[...][:, None], shape).reshape(useful * each, HS)

        def store(p, value):
            out_ref[:, :, :, p * HS : (p + 1) * HS] = value.reshape(shape)

        rotate_store(sum_ref[...] * scale, cosine, sine, store)


def image_qkv_of(chunks, mine, cosine, sine, w_proj, bias, gain, all_qkv):
    groups = len(chunks)
    useful = cosine.shape[0]
    tiles, local_rows, depth = chunks[0].shape
    model_width, outs = all_qkv.shape
    each = tiles * local_rows
    block = 1024
    fixed = lambda *shape: pl.BlockSpec(shape, lambda i, c: (0,) * len(shape))
    return pl.pallas_call(
        functools.partial(image_kernel, groups=groups, useful=useful),
        grid_spec=pltpu.PrefetchScalarGridSpec(
            num_scalar_prefetch=1,
            grid=(model_width // block,),
            in_specs=[fixed(tiles, local_rows, depth)] * groups
            + [
                fixed(useful, local_rows, HS),
                fixed(useful, local_rows, HS),
                pl.BlockSpec((depth, block), lambda i, c: (0, i)),
                pl.BlockSpec((1, block), lambda i, c: (0, i)),
                pl.BlockSpec((1, block), lambda i, c: (0, i)),
                pl.BlockSpec((block, outs), lambda i, c: (i, 0)),
            ],
            out_specs=[
                fixed(useful, tiles, local_rows, outs),
                pl.BlockSpec((each, block), lambda i, c: (0, i)),
            ],
            scratch_shapes=[
                pltpu.VMEM((useful * each, depth), jnp.bfloat16),
                pltpu.VMEM((useful * each, outs), jnp.float32),
                pltpu.VMEM((useful * each, 1), jnp.float32),
            ],
        ),
        out_shape=[
            jax.ShapeDtypeStruct((useful, tiles, local_rows, outs), jnp.bfloat16),
            jax.ShapeDtypeStruct((each, model_width), jnp.bfloat16),
        ],
        compiler_params=pltpu.CompilerParams(dimension_semantics=("arbitrary",)),
        cost_estimate=pl.CostEstimate(
            flops=2 * useful * each * model_width * (depth + outs),
            bytes_accessed=2 * model_width * (depth + outs),
            transcendentals=0,
        ),
    )(mine.reshape(1), *chunks, cosine, sine, w_proj, bias, gain, all_qkv)


def attend_kernel(counts_ref, image_ref, text_ref, out_ref):
    tile = pl.program_id(0)
    patch = counts_ref[0, tile]
    texts = counts_ref[1, tile]
    length = patch + texts
    useful, _, local_rows, outs = image_ref.shape
    parts = out_ref.shape[0]
    rows = parts * local_rows
    row = lax.broadcasted_iota(jnp.int32, (rows, WINDOW), 0)
    place = lax.broadcasted_iota(jnp.int32, (rows, WINDOW), 1)
    placing = jnp.where((row == patch + place) & (place < texts), 1.0, 0.0).astype(jnp.bfloat16)
    placed = jnp.dot(placing, text_ref[...], preferred_element_type=jnp.float32)
    first = useful * local_rows
    image_row = lax.broadcasted_iota(jnp.int32, (first, outs), 0) < patch
    image = image_ref[...].reshape(first, outs).astype(jnp.float32)
    qkv = jnp.concatenate(
        [jnp.where(image_row, image, placed[:first]), placed[first:]], axis=0
    ).astype(jnp.bfloat16)
    keys = qkv[:, GROUP * HS : (GROUP + 1) * HS]
    values = qkv[:, (GROUP + 1) * HS :]
    at_row = lax.broadcasted_iota(jnp.int32, (rows, rows), 0)
    at_col = lax.broadcasted_iota(jnp.int32, (rows, rows), 1)
    allowed = (at_col <= at_row) & (at_col < length)
    for g in range(GROUP):
        scores = lax.dot_general(
            qkv[:, g * HS : (g + 1) * HS],
            keys,
            (((1,), (1,)), ((), ())),
            preferred_element_type=jnp.float32,
        ) * (1.0 / math.sqrt(HS))
        scores = jnp.where(allowed, scores, -1e30)
        row_max = jnp.max(scores, axis=1, keepdims=True)
        weights = jnp.where(allowed, jnp.exp(scores - row_max), 0.0)
        probabilities = (weights / jnp.sum(weights, axis=1, keepdims=True)).astype(jnp.bfloat16)
        attended = jnp.dot(probabilities, values, preferred_element_type=jnp.float32)
        out_ref[:, :, :, g * HS : (g + 1) * HS] = attended.astype(jnp.bfloat16).reshape(
            parts, 1, local_rows, HS
        )


def attend(image_qkv, text_qkv, counts, parts):
    useful, tiles, local_rows, outs = image_qkv.shape
    rows = parts * local_rows
    return pl.pallas_call(
        attend_kernel,
        grid_spec=pltpu.PrefetchScalarGridSpec(
            num_scalar_prefetch=1,
            grid=(tiles,),
            in_specs=[
                pl.BlockSpec((useful, 1, local_rows, outs), lambda t, c: (0, t, 0, 0)),
                pl.BlockSpec((WINDOW, outs), lambda t, c: (t, 0)),
            ],
            out_specs=pl.BlockSpec((parts, 1, local_rows, GROUP * HS), lambda t, c: (0, t, 0, 0)),
        ),
        out_shape=jax.ShapeDtypeStruct((parts, tiles, local_rows, GROUP * HS), jnp.bfloat16),
        compiler_params=pltpu.CompilerParams(dimension_semantics=("arbitrary",)),
        cost_estimate=pl.CostEstimate(
            flops=tiles * rows * (2 * WINDOW * outs + 4 * GROUP * rows * HS),
            bytes_accessed=4 * tiles * rows * outs,
            transcendentals=tiles * GROUP * rows * rows,
        ),
    )(counts, image_qkv, text_qkv)


def out_kernel(att_ref, weight_hbm, hidden_ref, out_ref, rows_ref, weight_ref, sems):
    heads, _, head_width = att_ref.shape
    blocks, _, width = weight_ref.shape
    pieces = sems.shape[0]
    each = blocks // pieces
    copies = [
        pltpu.make_async_copy(
            weight_hbm.at[i * each : (i + 1) * each],
            weight_ref.at[i * each : (i + 1) * each],
            sems.at[i],
        )
        for i in range(pieces)
    ]
    for copy in copies:
        copy.start()
    for h in range(heads):
        rows_ref[:, h * head_width : (h + 1) * head_width] = att_ref[h]
    for i, copy in enumerate(copies):
        copy.wait()
        weights = jnp.concatenate([weight_ref[i * each + j] for j in range(each)], axis=1)
        total = jnp.dot(rows_ref[...], weights, preferred_element_type=jnp.float32)
        cols = slice(i * each * width, (i + 1) * each * width)
        out_ref[:, cols] = (hidden_ref[:, cols].astype(jnp.float32) + total).astype(jnp.bfloat16)


def project_out(attended, weight_blocks, hidden):
    _, rows, _ = attended.shape
    blocks, depth, width = weight_blocks.shape
    whole = pl.BlockSpec(memory_space=pltpu.VMEM)
    return pl.pallas_call(
        out_kernel,
        in_specs=[whole, pl.BlockSpec(memory_space=pl.ANY), whole],
        out_specs=whole,
        out_shape=jax.ShapeDtypeStruct((rows, blocks * width), jnp.bfloat16),
        scratch_shapes=[
            pltpu.VMEM((rows, depth), jnp.bfloat16),
            pltpu.VMEM((blocks, depth, width), jnp.bfloat16),
            pltpu.SemaphoreType.DMA((blocks // 4,)),
        ],
        cost_estimate=pl.CostEstimate(
            flops=2 * rows * depth * blocks * width,
            bytes_accessed=2 * depth * blocks * width,
            transcendentals=0,
        ),
    )(attended, weight_blocks, hidden)


def body(
    vit_features,
    patch_counts,
    text_counts,
    tile_dest,
    text_embeds,
    w_proj,
    b_proj,
    norm_gain,
    w_qkv,
    w_out,
):
    parts = lax.axis_size("mp")
    mine = lax.axis_index("mp")
    image_count, local_rows, _ = vit_features.shape
    model_width = text_embeds.shape[-1]
    slice_width = model_width // parts
    each = image_count * local_rows
    lengths = patch_counts + text_counts
    counts = jnp.stack([patch_counts, text_counts, jnp.full((image_count,), mine, jnp.int32)])

    all_qkv = lax.all_gather(w_qkv[0, :, 0], "dp", axis=0, tiled=True)

    payload = pack(text_embeds, w_out[0, 0], mine, parts)
    got = [payload[0]] + [shifted(payload[s], "mp", s) for s in range(1, parts)]
    window, all_heads = unpack(got, counts, image_count, slice_width, w_out.shape[3])
    all_out = lax.all_gather(all_heads[None], "dp", axis=0, tiled=True)

    arrived = exchange_tiles(vit_features, tile_dest)
    chunks = ring_chunks(arrived, "mp", -(-IMAGE_ROWS // local_rows))
    text_chunks = ring_chunks(window, "mp")

    text_places = patch_counts[:, None] + jnp.arange(WINDOW, dtype=jnp.int32)[None, :]
    text_cos, text_sin = rotation_tables(text_places.reshape(-1))
    local = jnp.arange(local_rows, dtype=jnp.int32)
    useful = -(-IMAGE_ROWS // local_rows)
    chunk_cos, chunk_sin = rotation_tables(
        jnp.arange(useful * local_rows, dtype=jnp.int32).reshape(useful, local_rows)
    )

    bias = b_proj.reshape(1, model_width)
    image_qkv, own_projected = image_qkv_of(
        chunks, mine, chunk_cos, chunk_sin, w_proj, bias, norm_gain, all_qkv
    )
    text_qkv = text_qkv_of(text_chunks, mine, text_cos, text_sin, norm_gain, all_qkv)

    own_rows = (mine * local_rows + local)[None, :, None]
    hidden = jnp.where(
        own_rows < patch_counts[:, None, None],
        own_projected.reshape(image_count, local_rows, model_width),
        jnp.where(
            own_rows < lengths[:, None, None], text_embeds, jnp.zeros_like(text_embeds)
        ),
    ).reshape(each, model_width)

    attended = attend(image_qkv, text_qkv, counts, parts)
    returned = lax.all_to_all(
        attended.reshape(parts, each, -1), "mp", split_axis=0, concat_axis=0, tiled=True
    )
    out = project_out(returned, all_out, hidden)
    return out.reshape(image_count, local_rows, model_width)


def solution(mesh):
    in_specs = (
        P("dp", "mp", None),
        P("dp"),
        P("dp"),
        P("dp"),
        P("dp", "mp", None),
        P(),
        P(),
        P(),
        P(None, "dp", "mp", None),
        P(None, "mp", None, "dp"),
    )
    out_specs = P("dp", "mp", None)

    return jax.shard_map(body, mesh=mesh, in_specs=in_specs, out_specs=out_specs, check_vma=False)
```

```python
import functools
import math

import jax
import jax.numpy as jnp
from jax import lax
from jax.experimental import pallas as pl
from jax.experimental.pallas import tpu as pltpu
from jax.sharding import PartitionSpec as P


HS = 128
GROUP = 2
WINDOW = 64
IMAGE_ROWS = 192
EXTRA = 128

rope_base = 500000.0
epsilon = 1e-05


def shifted(value, axis, step, sources=None):
    size = lax.axis_size(axis)
    pairs = [(i, (i + step) % size) for i in range(size) if sources is None or i in sources]
    return lax.ppermute(value, axis, pairs)


def ring_chunks(own, axis, useful=None):
    size = lax.axis_size(axis)
    useful = size if useful is None else useful
    chunks = [own] + [None] * (size - 1)
    for s in range(1, size // 2 + 1):
        holders = [(o + s - 1) % size for o in range(useful)]
        chunks[s] = shifted(chunks[s - 1], axis, 1, holders)
        if s < size - s:
            holders = [(o - s + 1) % size for o in range(useful)]
            chunks[size - s] = shifted(chunks[(size - s + 1) % size], axis, -1, holders)
    return chunks


def rotation_tables(rows):
    half_size = HS // 2
    inverse = jnp.exp(
        -(2.0 * jnp.arange(half_size, dtype=jnp.float32) / HS) * math.log(rope_base)
    )
    angles = rows.astype(jnp.float32)[..., None] * inverse
    cosine, sine = jnp.cos(angles), jnp.sin(angles)
    return (
        jnp.concatenate([cosine, cosine], axis=-1),
        jnp.concatenate([-sine, sine], axis=-1),
    )


def rotate_store(joined, cosine, sine, store):
    heads = joined.shape[1] // HS
    for p in range(heads):
        part = joined[:, p * HS : (p + 1) * HS]
        if p < heads - 1:
            part = part * cosine + pltpu.roll(part, HS // 2, 1) * sine
        store(p, part.astype(jnp.bfloat16))


def order_kernel(got_ref, out_ref, *, image_count):
    total, wide = got_ref.shape
    width = wide - EXTRA
    dest = got_ref[:, width:].astype(jnp.float32)
    row = lax.broadcasted_iota(jnp.int32, (total, total), 0)
    col = lax.broadcasted_iota(jnp.int32, (total, total), 1)
    earlier = (dest == dest.T) & (col < row)
    slots = jnp.sum(jnp.where(earlier, 1.0, 0.0), axis=1, keepdims=True)
    targets = (dest * image_count + slots).T
    placing = jnp.where(targets == row.astype(jnp.float32), 1.0, 0.0).astype(jnp.bfloat16)
    out_ref[...] = jnp.dot(
        placing, got_ref[:, :width], preferred_element_type=jnp.float32
    ).astype(jnp.bfloat16)


def exchange_tiles(vit_features, tile_dest):
    image_count, _, width = vit_features.shape
    ranks = lax.axis_size("dp")
    by_row = jnp.moveaxis(vit_features, 1, 0)
    tags = jnp.broadcast_to(
        tile_dest.astype(jnp.bfloat16)[None, :, None], (ranks, image_count, EXTRA)
    )
    sent = jnp.concatenate([by_row, tags], axis=2)
    got = lax.all_to_all(sent, "dp", split_axis=0, concat_axis=0, tiled=True)
    total = ranks * image_count
    ordered = pl.pallas_call(
        functools.partial(order_kernel, image_count=image_count),
        out_shape=jax.ShapeDtypeStruct((total, width), jnp.bfloat16),
        cost_estimate=pl.CostEstimate(
            flops=2 * total * total * width, bytes_accessed=4 * total * width, transcendentals=0
        ),
    )(got.reshape(total, width + EXTRA))
    arrived = lax.all_to_all(
        ordered.reshape(ranks, image_count, width),
        "dp",
        split_axis=0,
        concat_axis=0,
        tiled=True,
    )
    return jnp.moveaxis(arrived, 0, 1)


def pack_kernel(place_ref, text_ref, heads_ref, *out_refs):
    parts = len(out_refs)
    rows, wide = out_refs[0].shape
    folds = heads_ref.shape[0] // rows
    cols = heads_ref.shape[1]
    width = wide - folds * cols
    mine = place_ref[0]
    for s, out_ref in enumerate(out_refs):
        at = pl.multiple_of(lax.rem(mine + s, parts) * width, width)
        out_ref[:, :width] = text_ref[:, :, pl.ds(at, width)].reshape(rows, width)
        for f in range(folds):
            out_ref[:, width + f * cols : width + (f + 1) * cols] = heads_ref[
                f * rows : (f + 1) * rows, :
            ]


def pack(text_embeds, head_rows, mine, parts):
    tiles, local_rows, model_width = text_embeds.shape
    rows = tiles * local_rows
    width = model_width // parts
    wide = width + head_rows.shape[0] * head_rows.shape[1] // rows
    whole = pl.BlockSpec(memory_space=pltpu.VMEM)
    return pl.pallas_call(
        pack_kernel,
        in_specs=[pl.BlockSpec(memory_space=pltpu.SMEM), whole, whole],
        out_specs=[whole] * parts,
        out_shape=[jax.ShapeDtypeStruct((rows, wide), jnp.bfloat16)] * parts,
        cost_estimate=pl.CostEstimate(
            flops=1 << 20, bytes_accessed=4 * parts * rows * wide, transcendentals=0
        ),
    )(mine.reshape(1), text_embeds, head_rows)


def unpack_kernel(counts_ref, *refs, tiles, width):
    parts = len(refs) - 3
    got_refs = refs[:parts]
    window_ref, heads_ref, rows_ref = refs[parts:]
    mine = counts_ref[2, 0]
    each, wide = got_refs[0].shape
    local_rows = each // tiles
    cols = heads_ref.shape[1]
    folds = (wide - width) // cols
    for s, got_ref in enumerate(got_refs):
        at = lax.rem(mine + (parts - s), parts)
        for f in range(folds):
            begin = pl.multiple_of((at * folds + f) * each, each)
            heads_ref[pl.ds(begin, each), :] = got_ref[:, width + f * cols : width + (f + 1) * cols]
        for t in range(tiles):
            rows_ref[t, at] = got_ref[t * local_rows : (t + 1) * local_rows, :width]
    rows = parts * local_rows
    place = lax.broadcasted_iota(jnp.int32, (WINDOW, rows), 0)
    row = lax.broadcasted_iota(jnp.int32, (WINDOW, rows), 1)
    for t in range(tiles):
        picks = (row == counts_ref[0, t] + place) & (place < counts_ref[1, t])
        window_ref[t * WINDOW : (t + 1) * WINDOW, :] = jnp.dot(
            jnp.where(picks, 1.0, 0.0).astype(jnp.bfloat16),
            rows_ref[t].reshape(rows, width),
            preferred_element_type=jnp.float32,
        ).astype(jnp.bfloat16)


def unpack(got, counts, tiles, width, cols):
    parts = len(got)
    each, wide = got[0].shape
    local_rows = each // tiles
    whole = pl.BlockSpec(memory_space=pltpu.VMEM)
    return pl.pallas_call(
        functools.partial(unpack_kernel, tiles=tiles, width=width),
        in_specs=[pl.BlockSpec(memory_space=pltpu.SMEM)] + [whole] * parts,
        out_specs=[whole, whole],
        out_shape=[
            jax.ShapeDtypeStruct((tiles * WINDOW, width), jnp.bfloat16),
            jax.ShapeDtypeStruct((parts * each * ((wide - width) // cols), cols), jnp.bfloat16),
        ],
        scratch_shapes=[pltpu.VMEM((tiles, parts, local_rows, width), jnp.bfloat16)],
        cost_estimate=pl.CostEstimate(
            flops=2 * tiles * WINDOW * parts * local_rows * width,
            bytes_accessed=2 * parts * each * wide,
            transcendentals=0,
        ),
    )(counts, *got)


def text_kernel(place_ref, *refs):
    parts = len(refs) - 7
    chunk_refs = refs[:parts]
    cos_ref, sin_ref, gain_ref, weight_hbm, out_ref, weight_ref, sems = refs[parts:]
    width = chunk_refs[0].shape[1]
    mine = place_ref[0]
    copies = []
    for s in range(parts):
        begin = pl.multiple_of(lax.rem(mine + (parts - s), parts) * width, width)
        copies.append(
            pltpu.make_async_copy(
                weight_hbm.at[pl.ds(begin, width)], weight_ref.at[s], sems.at[s]
            )
        )
    for copy in copies:
        copy.start()
    squares = None
    total = None
    for s, chunk_ref in enumerate(chunk_refs):
        at = lax.rem(mine + (parts - s), parts)
        rows = chunk_ref[...].astype(jnp.float32)
        part = jnp.sum(rows * rows, axis=1, keepdims=True)
        squares = part if squares is None else squares + part
        scaled = (rows * gain_ref[pl.ds(at, 1), :]).astype(jnp.bfloat16)
        copies[s].wait()
        term = jnp.dot(scaled, weight_ref[s], preferred_element_type=jnp.float32)
        total = term if total is None else total + term
    scale = lax.rsqrt(squares * (1.0 / (parts * width)) + epsilon)

    def store(p, value):
        out_ref[:, p * HS : (p + 1) * HS] = value

    rotate_store(total * scale, cos_ref[...], sin_ref[...], store)


def text_qkv_of(chunks, mine, cosine, sine, gain, all_qkv):
    rows, width = chunks[0].shape
    parts = len(chunks)
    outs = all_qkv.shape[1]
    whole = pl.BlockSpec(memory_space=pltpu.VMEM)
    return pl.pallas_call(
        text_kernel,
        in_specs=[pl.BlockSpec(memory_space=pltpu.SMEM)]
        + [whole] * (parts + 3)
        + [pl.BlockSpec(memory_space=pl.ANY)],
        out_specs=whole,
        out_shape=jax.ShapeDtypeStruct((rows, outs), jnp.bfloat16),
        scratch_shapes=[
            pltpu.VMEM((parts, width, outs), jnp.bfloat16),
            pltpu.SemaphoreType.DMA((parts,)),
        ],
        cost_estimate=pl.CostEstimate(
            flops=2 * rows * parts * width * outs,
            bytes_accessed=2 * parts * width * (rows + outs),
            transcendentals=0,
        ),
    )(mine.reshape(1), *chunks, cosine, sine, gain.reshape(parts, width), all_qkv)


def image_kernel(place_ref, *refs, groups, useful):
    chunk_refs = refs[:groups]
    cos_ref, sin_ref, proj_ref, bias_ref, gain_ref, qkv_ref = refs[groups : groups + 6]
    out_ref, hidden_ref, rows_ref, sum_ref, squares_ref = refs[groups + 6 :]
    tiles, local_rows, depth = chunk_refs[0].shape
    each = tiles * local_rows
    step = pl.program_id(0)
    mine = place_ref[0]

    @pl.when(step == 0)
    def _():
        for s, chunk_ref in enumerate(chunk_refs):
            at = lax.rem(mine + (groups - s), groups)

            @pl.when(at < useful)
            def _(at=at, chunk_ref=chunk_ref):
                begin = pl.multiple_of(at * each, each)
                rows_ref[pl.ds(begin, each), :] = chunk_ref[...].reshape(each, depth)

        sum_ref[...] = jnp.zeros_like(sum_ref)
        squares_ref[...] = jnp.zeros_like(squares_ref)

    projected = (
        jnp.dot(rows_ref[...], proj_ref[...], preferred_element_type=jnp.float32) + bias_ref[...]
    ).astype(jnp.bfloat16)
    for at in range(useful):

        @pl.when(mine == at)
        def _(at=at):
            hidden_ref[...] = projected[at * each : (at + 1) * each]

    @pl.when(mine >= useful)
    def _():
        hidden_ref[...] = jnp.zeros_like(hidden_ref)

    wide = projected.astype(jnp.float32)
    squares_ref[...] += jnp.sum(wide * wide, axis=1, keepdims=True)
    scaled = (wide * gain_ref[...]).astype(jnp.bfloat16)
    sum_ref[...] += jnp.dot(scaled, qkv_ref[...], preferred_element_type=jnp.float32)

    @pl.when(step == pl.num_programs(0) - 1)
    def _():
        model_width = proj_ref.shape[1] * pl.num_programs(0)
        scale = lax.rsqrt(squares_ref[...] * (1.0 / model_width) + epsilon)
        shape = (useful, tiles, local_rows, HS)
        cosine = jnp.broadcast_to(cos_ref[...][:, None], shape).reshape(useful * each, HS)
        sine = jnp.broadcast_to(sin_ref[...][:, None], shape).reshape(useful * each, HS)

        def store(p, value):
            out_ref[:, :, :, p * HS : (p + 1) * HS] = value.reshape(shape)

        rotate_store(sum_ref[...] * scale, cosine, sine, store)


def image_qkv_of(chunks, mine, cosine, sine, w_proj, bias, gain, all_qkv):
    groups = len(chunks)
    useful = cosine.shape[0]
    tiles, local_rows, depth = chunks[0].shape
    model_width, outs = all_qkv.shape
    each = tiles * local_rows
    block = 1024
    fixed = lambda *shape: pl.BlockSpec(shape, lambda i, c: (0,) * len(shape))
    return pl.pallas_call(
        functools.partial(image_kernel, groups=groups, useful=useful),
        grid_spec=pltpu.PrefetchScalarGridSpec(
            num_scalar_prefetch=1,
            grid=(model_width // block,),
            in_specs=[fixed(tiles, local_rows, depth)] * groups
            + [
                fixed(useful, local_rows, HS),
                fixed(useful, local_rows, HS),
                pl.BlockSpec((depth, block), lambda i, c: (0, i)),
                pl.BlockSpec((1, block), lambda i, c: (0, i)),
                pl.BlockSpec((1, block), lambda i, c: (0, i)),
                pl.BlockSpec((block, outs), lambda i, c: (i, 0)),
            ],
            out_specs=[
                fixed(useful, tiles, local_rows, outs),
                pl.BlockSpec((each, block), lambda i, c: (0, i)),
            ],
            scratch_shapes=[
                pltpu.VMEM((useful * each, depth), jnp.bfloat16),
                pltpu.VMEM((useful * each, outs), jnp.float32),
                pltpu.VMEM((useful * each, 1), jnp.float32),
            ],
        ),
        out_shape=[
            jax.ShapeDtypeStruct((useful, tiles, local_rows, outs), jnp.bfloat16),
            jax.ShapeDtypeStruct((each, model_width), jnp.bfloat16),
        ],
        compiler_params=pltpu.CompilerParams(dimension_semantics=("arbitrary",)),
        cost_estimate=pl.CostEstimate(
            flops=2 * useful * each * model_width * (depth + outs),
            bytes_accessed=2 * model_width * (depth + outs),
            transcendentals=0,
        ),
    )(mine.reshape(1), *chunks, cosine, sine, w_proj, bias, gain, all_qkv)


def attend_kernel(counts_ref, image_ref, text_ref, out_ref):
    tile = pl.program_id(0)
    patch = counts_ref[0, tile]
    texts = counts_ref[1, tile]
    length = patch + texts
    useful, _, local_rows, outs = image_ref.shape
    parts = out_ref.shape[0]
    rows = parts * local_rows
    row = lax.broadcasted_iota(jnp.int32, (rows, WINDOW), 0)
    place = lax.broadcasted_iota(jnp.int32, (rows, WINDOW), 1)
    placing = jnp.where((row == patch + place) & (place < texts), 1.0, 0.0).astype(jnp.bfloat16)
    placed = jnp.dot(placing, text_ref[...], preferred_element_type=jnp.float32)
    first = useful * local_rows
    image_row = lax.broadcasted_iota(jnp.int32, (first, outs), 0) < patch
    image = image_ref[...].reshape(first, outs).astype(jnp.float32)
    qkv = jnp.concatenate(
        [jnp.where(image_row, image, placed[:first]), placed[first:]], axis=0
    ).astype(jnp.bfloat16)
    keys = qkv[:, GROUP * HS : (GROUP + 1) * HS]
    values = qkv[:, (GROUP + 1) * HS :]
    at_row = lax.broadcasted_iota(jnp.int32, (rows, rows), 0)
    at_col = lax.broadcasted_iota(jnp.int32, (rows, rows), 1)
    allowed = (at_col <= at_row) & (at_col < length)
    for g in range(GROUP):
        scores = lax.dot_general(
            qkv[:, g * HS : (g + 1) * HS],
            keys,
            (((1,), (1,)), ((), ())),
            preferred_element_type=jnp.float32,
        ) * (1.0 / math.sqrt(HS))
        scores = jnp.where(allowed, scores, -1e30)
        row_max = jnp.max(scores, axis=1, keepdims=True)
        weights = jnp.exp(scores - row_max)
        share = 1.0 / jnp.sum(weights, axis=1, keepdims=True)
        probabilities = (weights * share).astype(jnp.bfloat16)
        attended = jnp.dot(probabilities, values, preferred_element_type=jnp.float32)
        out_ref[:, :, :, g * HS : (g + 1) * HS] = attended.astype(jnp.bfloat16).reshape(
            parts, 1, local_rows, HS
        )


def attend(image_qkv, text_qkv, counts, parts):
    useful, tiles, local_rows, outs = image_qkv.shape
    rows = parts * local_rows
    return pl.pallas_call(
        attend_kernel,
        grid_spec=pltpu.PrefetchScalarGridSpec(
            num_scalar_prefetch=1,
            grid=(tiles,),
            in_specs=[
                pl.BlockSpec((useful, 1, local_rows, outs), lambda t, c: (0, t, 0, 0)),
                pl.BlockSpec((WINDOW, outs), lambda t, c: (t, 0)),
            ],
            out_specs=pl.BlockSpec((parts, 1, local_rows, GROUP * HS), lambda t, c: (0, t, 0, 0)),
        ),
        out_shape=jax.ShapeDtypeStruct((parts, tiles, local_rows, GROUP * HS), jnp.bfloat16),
        compiler_params=pltpu.CompilerParams(dimension_semantics=("arbitrary",)),
        cost_estimate=pl.CostEstimate(
            flops=tiles * rows * (2 * WINDOW * outs + 4 * GROUP * rows * HS),
            bytes_accessed=4 * tiles * rows * outs,
            transcendentals=tiles * GROUP * rows * rows,
        ),
    )(counts, image_qkv, text_qkv)


def out_kernel(att_ref, weight_hbm, hidden_ref, out_ref, rows_ref, weight_ref, sems):
    heads, _, head_width = att_ref.shape
    blocks, _, width = weight_ref.shape
    pieces = sems.shape[0]
    each = blocks // pieces
    copies = [
        pltpu.make_async_copy(
            weight_hbm.at[i * each : (i + 1) * each],
            weight_ref.at[i * each : (i + 1) * each],
            sems.at[i],
        )
        for i in range(pieces)
    ]
    for copy in copies:
        copy.start()
    for h in range(heads):
        rows_ref[:, h * head_width : (h + 1) * head_width] = att_ref[h]
    for i, copy in enumerate(copies):
        copy.wait()
        weights = jnp.concatenate([weight_ref[i * each + j] for j in range(each)], axis=1)
        total = jnp.dot(rows_ref[...], weights, preferred_element_type=jnp.float32)
        cols = slice(i * each * width, (i + 1) * each * width)
        out_ref[:, cols] = (hidden_ref[:, cols].astype(jnp.float32) + total).astype(jnp.bfloat16)


def project_out(attended, weight_blocks, hidden):
    _, rows, _ = attended.shape
    blocks, depth, width = weight_blocks.shape
    whole = pl.BlockSpec(memory_space=pltpu.VMEM)
    return pl.pallas_call(
        out_kernel,
        in_specs=[whole, pl.BlockSpec(memory_space=pl.ANY), whole],
        out_specs=whole,
        out_shape=jax.ShapeDtypeStruct((rows, blocks * width), jnp.bfloat16),
        scratch_shapes=[
            pltpu.VMEM((rows, depth), jnp.bfloat16),
            pltpu.VMEM((blocks, depth, width), jnp.bfloat16),
            pltpu.SemaphoreType.DMA((blocks // 4,)),
        ],
        cost_estimate=pl.CostEstimate(
            flops=2 * rows * depth * blocks * width,
            bytes_accessed=2 * depth * blocks * width,
            transcendentals=0,
        ),
    )(attended, weight_blocks, hidden)


def body(
    vit_features,
    patch_counts,
    text_counts,
    tile_dest,
    text_embeds,
    w_proj,
    b_proj,
    norm_gain,
    w_qkv,
    w_out,
):
    parts = lax.axis_size("mp")
    mine = lax.axis_index("mp")
    image_count, local_rows, _ = vit_features.shape
    model_width = text_embeds.shape[-1]
    slice_width = model_width // parts
    each = image_count * local_rows
    lengths = patch_counts + text_counts
    counts = jnp.stack([patch_counts, text_counts, jnp.full((image_count,), mine, jnp.int32)])

    all_qkv = lax.all_gather(w_qkv[0, :, 0], "dp", axis=0, tiled=True)

    payload = pack(text_embeds, w_out[0, 0], mine, parts)
    got = [payload[0]] + [shifted(payload[s], "mp", s) for s in range(1, parts)]
    window, all_heads = unpack(got, counts, image_count, slice_width, w_out.shape[3])
    all_out = lax.all_gather(all_heads[None], "dp", axis=0, tiled=True)

    arrived = exchange_tiles(vit_features, tile_dest)
    chunks = ring_chunks(arrived, "mp", -(-IMAGE_ROWS // local_rows))
    text_chunks = ring_chunks(window, "mp")

    text_places = patch_counts[:, None] + jnp.arange(WINDOW, dtype=jnp.int32)[None, :]
    text_cos, text_sin = rotation_tables(text_places.reshape(-1))
    local = jnp.arange(local_rows, dtype=jnp.int32)
    useful = -(-IMAGE_ROWS // local_rows)
    chunk_cos, chunk_sin = rotation_tables(
        jnp.arange(useful * local_rows, dtype=jnp.int32).reshape(useful, local_rows)
    )

    bias = b_proj.reshape(1, model_width)
    image_qkv, own_projected = image_qkv_of(
        chunks, mine, chunk_cos, chunk_sin, w_proj, bias, norm_gain, all_qkv
    )
    text_qkv = text_qkv_of(text_chunks, mine, text_cos, text_sin, norm_gain, all_qkv)

    own_rows = (mine * local_rows + local)[None, :, None]
    hidden = jnp.where(
        own_rows < patch_counts[:, None, None],
        own_projected.reshape(image_count, local_rows, model_width),
        jnp.where(
            own_rows < lengths[:, None, None], text_embeds, jnp.zeros_like(text_embeds)
        ),
    ).reshape(each, model_width)

    attended = attend(image_qkv, text_qkv, counts, parts)
    returned = lax.all_to_all(
        attended.reshape(parts, each, -1), "mp", split_axis=0, concat_axis=0, tiled=True
    )
    out = project_out(returned, all_out, hidden)
    return out.reshape(image_count, local_rows, model_width)


def solution(mesh):
    in_specs = (
        P("dp", "mp", None),
        P("dp"),
        P("dp"),
        P("dp"),
        P("dp", "mp", None),
        P(),
        P(),
        P(),
        P(None, "dp", "mp", None),
        P(None, "mp", None, "dp"),
    )
    out_specs = P("dp", "mp", None)

    return jax.shard_map(body, mesh=mesh, in_specs=in_specs, out_specs=out_specs, check_vma=False)
```
